128 devices in a mesh: dp: 16 (over y, x), seq: 8 (over z, core).
Axes of the slice: x: 4, y: 4, z: 4, core: 2. Of those that a mesh axis runs over, the one named last changes fastest.
Arguments:
- hidden_in: bfloat16 [16, 1024, 2048], P('dp', 'seq'), may hold values from -6 to 6
- cotangent: bfloat16 [16, 1024, 2048], P('dp', 'seq'), may hold values from -6 to 6
- norm_gain: float32 [2048], P('dp'), may hold values from 0.1 to 1.9
- route_weights: float32 [16, 1024, 10], P('dp', 'seq'), may hold values from 0.1 to 1
- expert_ids: int32 [16, 1024, 10], P('dp', 'seq'), may hold values from 0 to 255, all different within a row; in each aligned block of 128 rows (0 to 127, 128 to 255, ..., all dimensions but the last counted through in order) at most 6 rows name the same one
- expert_gate: bfloat16 [256, 2048, 512], P(('dp', 'seq')), may hold values from -0.125 to 0.125
- expert_up: bfloat16 [256, 2048, 512], P(('dp', 'seq')), may hold values from -0.125 to 0.125
- expert_down: bfloat16 [256, 512, 2048], P(('dp', 'seq')), may hold values from -0.25 to 0.25
Outputs:
- grad_hidden: bfloat16 [16, 1024, 2048], P('dp', 'seq')
- grad_gain: float32 [2048], P('dp')
- grad_gate: bfloat16 [256, 2048, 512], P(('dp', 'seq'))
- grad_up: bfloat16 [256, 2048, 512], P(('dp', 'seq'))
- grad_down: bfloat16 [256, 512, 2048], P(('dp', 'seq'))
The draws below stay inside these ranges and needn't reach their ends.
Inputs may be any that keep to these rules, and one draw needn't show every extreme that they name: `expert_ids`: each token names 10 different experts. Among the rows of one device no expert is named by more than 6 of them, and in some device one expert is named by exactly 6.
All inputs are finite; a program needn't handle non-finite values.
Results may differ from the reference program's by a relative error of at most 0.0072.
Values may be sent and summed in bfloat16 or wider, within the bound.
A program may use at most 192 MiB of HBM per device.

```python
import math
import jax
import jax.numpy as jnp
import numpy as np
from jax import lax

D = 2048
HIDDEN_SIZE = 512
TOP = 10
TOK_DEV = 128
SEQS = 16
LEN = 1024
EXPERTS = 256
CAP = 6
N_DP = 16
N_SEQ = 8


def block_scale(key, dims, pieces, least, high):
    level = 1.0
    for axis_at, shards_of in pieces:
        draws = jax.random.uniform(jax.random.fold_in(jax.random.fold_in(key, 6), axis_at), (shards_of,), jnp.float32, least / len(pieces), high / len(pieces))
        level = level * jnp.repeat(jnp.exp(draws), dims[axis_at] // shards_of).reshape((-1,) + (1,) * (len(dims) - 1 - axis_at))
    return level


def shared_out(key, own, number, rows, amount, top, reach, slope):
    order = jax.random.permutation(key, amount)
    heavy_load, ordinary = portions_of(amount, rows * top, reach, slope, True), portions_of(amount, rows * top, reach, slope, False)
    places = jnp.arange(amount)

    def named(lengths, rotation):
        used = int((lengths > 0).sum())
        fixed = max(1, used // 4)
        shifted = fixed + (places - fixed + rotation * (used - fixed)) % max(1, amount - fixed)
        return jnp.zeros((amount,), jnp.int32).at[order[jnp.where(places < fixed, places, shifted)]].set(jnp.asarray(lengths, jnp.int32))

    lengths = jnp.where(number % 4 == 0, named(heavy_load, number // 4), named(ordinary, number - number // 4 - 1))
    mixed = jax.random.permutation(jax.random.fold_in(own, 3), amount)
    giver, sink = mixed[0:amount // 2 * 2:2], mixed[1:amount // 2 * 2:2]
    room = jnp.minimum(lengths[giver] - 1, reach - lengths[sink]) // 2
    room = jnp.where((giver == order[0]) | (sink == order[0]) | (lengths[sink] == 0), 0, jnp.maximum(room, 0))
    shifted = jax.random.randint(jax.random.fold_in(own, 4), (amount // 2,), 0, 1 << 20) % (room + 1)
    lengths = lengths.at[giver].add(-shifted).at[sink].add(shifted)
    members = jnp.searchsorted(jnp.cumsum(lengths), jnp.arange(rows * top), side="right").astype(jnp.int32)
    grid = members.reshape(top, rows).T
    grid = grid[jax.random.permutation(jax.random.fold_in(own, 1), rows)]
    rotation = jax.random.randint(jax.random.fold_in(own, 2), (rows, 1), 0, top)
    return jnp.take_along_axis(grid, (jnp.arange(top)[None, :] + rotation) % top, axis=1)


def portions_of(count, total, limit, skew, full):
    portions = [(1 << 20) // math.isqrt(rank ** skew) + 1 for rank in range(1, count + 1)]
    largest = limit if full else min(limit, max(-(-total // count), total * portions[0] // sum(portions)))
    least = 1 if total - largest >= count - 1 else 0
    given, rest = [largest] + [least] * (count - 1), total - largest - least * (count - 1)
    while rest > 0:
        candidates = [i for i in range(1, count) if given[i] < largest] or [i for i in range(1, count) if given[i] < limit]
        whole, left = sum([portions[i] for i in candidates]), rest
        for i in candidates:
            addition = min(limit - given[i], max(1, left * portions[i] // whole), rest)
            given[i] = given[i] + addition
            rest = rest - addition
    return np.array(given)


def normal_values(rng, shape, spread, bound, cuts=(), kind=jnp.bfloat16):
    array = jax.random.normal(rng, shape, jnp.float32) * spread
    if len(cuts) > 0:
        array = block_scale(rng, shape, cuts, -0.22, 0.18) * array
    return jnp.clip(array, min=-bound, max=bound).astype(kind)


def setup_inputs(seed: int = 0) -> dict:
    key_list = jax.random.split(jax.random.key(seed), 9)
    hidden_in = normal_values(key_list[0], (SEQS, LEN, D), 1.0, 6.0, ((0, 16), (1, 8)))
    cotangent = normal_values(key_list[1], (SEQS, LEN, D), 1.0, 6.0, ((0, 16), (1, 8)))
    norm_gain = jnp.clip(1.0 + 0.18 * jax.random.normal(key_list[2], (D,), jnp.float32), 0.1, 1.9)
    route_weights = jnp.clip(jnp.exp(math.log(1.0) - 2.3025851 * jax.random.uniform(key_list[3], (SEQS, LEN, TOP), jnp.float32) ** block_scale(key_list[3], (SEQS, LEN, TOP), ((0, 16), (1, 8)), -0.2, 0.2)), 0.1, 1.0)
    expert_ids_keys = jax.random.split(jax.random.fold_in(key_list[4], 1), SEQS * LEN // TOK_DEV)
    expert_ids_turns = jax.random.permutation(jax.random.fold_in(key_list[4], 3), SEQS * LEN // TOK_DEV)
    expert_ids = jax.vmap(lambda own, number: shared_out(jax.random.fold_in(key_list[4], 2), own, number, TOK_DEV, EXPERTS, TOP, CAP, 2))(expert_ids_keys, expert_ids_turns).reshape((SEQS, LEN, TOP))
    expert_gate = normal_values(key_list[5], (EXPERTS, D, HIDDEN_SIZE), D ** -0.5, 0.125, ((0, 128),))
    expert_up = normal_values(key_list[6], (EXPERTS, D, HIDDEN_SIZE), D ** -0.5, 0.125, ((0, 128),))
    expert_down = normal_values(key_list[7], (EXPERTS, HIDDEN_SIZE, D), HIDDEN_SIZE ** -0.5, 0.25, ((0, 128),))
    return dict(hidden_in=hidden_in, cotangent=cotangent, norm_gain=norm_gain, route_weights=route_weights, expert_ids=expert_ids, expert_gate=expert_gate, expert_up=expert_up, expert_down=expert_down)


EPSILON = 1e-06

def block_slots(block_experts):
    flat_experts = block_experts.reshape(-1)
    onehot = (flat_experts[:, None] == jnp.arange(EXPERTS, dtype=jnp.int32)[None, :]).astype(jnp.float32)
    before = jnp.cumsum(onehot, axis=0) - onehot
    earlier_count = lax.optimization_barrier(jnp.sum(before * onehot, axis=1)).astype(jnp.int32)
    return flat_experts * CAP + earlier_count

def reference(hidden_in, cotangent, norm_gain, route_weights, expert_ids, expert_gate, expert_up, expert_down):
    blocks = N_DP * N_SEQ
    model_width = hidden_in.shape[-1]
    per_block = TOK_DEV * TOP
    inputs = hidden_in.reshape(blocks * TOK_DEV, model_width).astype(jnp.float32)
    inverse_root = lax.rsqrt(lax.optimization_barrier(jnp.mean(inputs * inputs, axis=1, keepdims=True)) + EPSILON)
    scaled = inputs * inverse_root
    normed = (scaled * norm_gain[None, :]).astype(jnp.bfloat16)
    upstream = cotangent.reshape(blocks * TOK_DEV, model_width)
    weights_flat = route_weights.reshape(blocks * per_block)
    slot_index = lax.map(block_slots, expert_ids.reshape(blocks, TOK_DEV, TOP))

    def fill_table(block_slot):
        return jnp.zeros((EXPERTS * CAP,), jnp.int32).at[block_slot].set(jnp.arange(per_block, dtype=jnp.int32) + 1)
    slot_table = jax.vmap(fill_table)(slot_index)
    slot_table = slot_table.reshape(blocks, EXPERTS, CAP).transpose(1, 0, 2).reshape(EXPERTS, blocks * CAP)
    block_of_row = jnp.arange(blocks * CAP, dtype=jnp.int32) // CAP

    def one_expert(packed):
        slot_entry, gate_matrix, up_matrix, down_matrix = packed
        occupied = slot_entry > 0
        within = jnp.maximum(slot_entry - 1, 0)
        assignment = block_of_row * per_block + within
        token_row = block_of_row * TOK_DEV + within // TOP
        rows_in = jnp.where(occupied[:, None], normed[token_row], jnp.zeros((), jnp.bfloat16))
        row_weight = jnp.where(occupied, weights_flat[assignment], jnp.zeros((), jnp.float32))
        rows_grad = (row_weight[:, None] * upstream[token_row].astype(jnp.float32)).astype(jnp.bfloat16)
        pre_gate = jnp.dot(rows_in, gate_matrix, preferred_element_type=jnp.float32)
        pre_up = jnp.dot(rows_in, up_matrix, preferred_element_type=jnp.float32)
        sigmoid_gate = jax.nn.sigmoid(pre_gate)
        silu_gate = pre_gate * sigmoid_gate
        activation = (silu_gate * pre_up).astype(jnp.bfloat16)
        grad_act = jnp.dot(rows_grad, down_matrix.T, preferred_element_type=jnp.float32)
        gate_back = (grad_act * pre_up * sigmoid_gate * (1.0 + pre_gate * (1.0 - sigmoid_gate))).astype(jnp.bfloat16)
        up_back = (grad_act * silu_gate).astype(jnp.bfloat16)
        down_grad = jnp.dot(activation.T, rows_grad, preferred_element_type=jnp.float32).astype(jnp.bfloat16)
        gate_grad = jnp.dot(rows_in.T, gate_back, preferred_element_type=jnp.float32).astype(jnp.bfloat16)
        up_grad = jnp.dot(rows_in.T, up_back, preferred_element_type=jnp.float32).astype(jnp.bfloat16)
        returned = (jnp.dot(gate_back, gate_matrix.T, preferred_element_type=jnp.float32) + jnp.dot(up_back, up_matrix.T, preferred_element_type=jnp.float32)).astype(jnp.bfloat16)
        return (gate_grad, up_grad, down_grad, returned)
    grad_gate, grad_up, grad_down, returned = lax.map(one_expert, (slot_table, expert_gate, expert_up, expert_down))
    flat_back = returned.reshape(EXPERTS * blocks * CAP, model_width)

    def gather_block(packed):
        block_number, block_slot = packed
        where_rows = block_slot // CAP * (blocks * CAP) + block_number * CAP + block_slot % CAP
        picked = flat_back[where_rows].astype(jnp.float32).reshape(TOK_DEV, TOP, model_width)
        return lax.optimization_barrier(jnp.sum(picked, axis=1))
    summed = lax.map(gather_block, (jnp.arange(blocks, dtype=jnp.int32), slot_index))
    summed = summed.reshape(blocks * TOK_DEV, model_width)
    grad_gain = lax.optimization_barrier(jnp.sum(summed * scaled, axis=0))
    gained = summed * norm_gain[None, :]
    centered = lax.optimization_barrier(jnp.mean(gained * scaled, axis=1, keepdims=True))
    grad_hidden = (upstream.astype(jnp.float32) + inverse_root * (gained - scaled * centered)).astype(jnp.bfloat16)
    return (grad_hidden.reshape(hidden_in.shape), grad_gain, grad_gate, grad_up, grad_down)
```

```python
import functools

import jax
import jax.numpy as jnp
import numpy as np
from jax import lax
from jax.experimental import pallas as pl
from jax.experimental.pallas import tpu as pltpu
from jax.sharding import PartitionSpec as P

TOP = 10
EPSILON = 1e-06
CAP = 6
BF = jnp.bfloat16
F32 = jnp.float32
VMEM_LIMIT = 60 * 2**20


def dot(a, b, ca=1, cb=0):
    return lax.dot_general(a, b, (((ca,), (cb,)), ((), ())), preferred_element_type=F32)


def dispatch_kernel(which, ids_ref, w_ref, hid_ref, cot_ref, send_ref, tab_ref, tab_s, wt_s, src_s):
    step = pl.program_id(0)
    tokens = hid_ref.shape[0]
    half = hid_ref.shape[1] // 2
    devices = tab_s.shape[0]

    @pl.when(step == 0)
    def _():
        expert = 2 * lax.broadcasted_iota(jnp.int32, (devices, tokens), 0) + which
        hit = jnp.zeros((devices, tokens), F32)
        weight = jnp.zeros((devices, tokens), F32)
        for k in range(TOP):
            same = ids_ref[k : k + 1, :] == expert
            hit = hit + jnp.where(same, 1.0, 0.0)
            weight = weight + jnp.where(same, w_ref[k : k + 1, :], 0.0)
        earlier = lax.broadcasted_iota(jnp.int32, (tokens, tokens), 0) < lax.broadcasted_iota(
            jnp.int32, (tokens, tokens), 1
        )
        rank = dot(hit.astype(BF), jnp.where(earlier, 1.0, 0.0).astype(BF))
        table = jnp.where(hit > 0.0, rank, -1.0)
        tab_s[...] = table
        tab_ref[...] = table.astype(BF)
        wt_s[...] = weight
        for h in range(2):
            src_s[h * 2 * tokens : h * 2 * tokens + tokens, :] = hid_ref[:, h * half : (h + 1) * half]
            src_s[h * 2 * tokens + tokens : (h + 1) * 2 * tokens, :] = cot_ref[:, h * half : (h + 1) * half]

    group = send_ref.shape[0] // 24
    at = pl.ds(pl.multiple_of(step * group, group), group)
    shape = (group, 24, tokens)
    table = jnp.broadcast_to(tab_s[at, :][:, None, :], shape)
    weight = jnp.broadcast_to(wt_s[at, :][:, None, :], shape)
    row = lax.broadcasted_iota(jnp.int32, shape, 1)
    in_half = jnp.where(row >= 12, 1, 0)
    row = row - 12 * in_half
    is_grad = jnp.where(row >= CAP, 1, 0)
    slot = (row - CAP * is_grad).astype(F32)
    flat = (group * 24, tokens)
    pick = jnp.where(table == slot, 1.0, 0.0)
    scale = jnp.sum(
        jnp.where(is_grad == 1, pick * weight, jnp.where(lax.broadcasted_iota(jnp.int32, shape, 2) == 0, 1.0, 0.0)),
        axis=2,
        keepdims=True,
    ).reshape(flat[0], 1)
    kind = 2 * in_half + is_grad
    pieces = [jnp.where(kind == m, pick, 0.0).reshape(flat).astype(BF) for m in range(4)]
    left = jnp.concatenate(pieces, axis=1)
    send_ref[...] = (dot(left, src_s[...]) * scale).astype(BF)


def dispatch(which, devices, ids_t, w_t, hidden, cot):
    tokens, width = hidden.shape
    steps = 8
    rows = devices * 24
    whole = lambda *s: pl.BlockSpec(s, lambda g: tuple(0 for _ in s))
    return pl.pallas_call(
        functools.partial(dispatch_kernel, which),
        grid=(steps,),
        out_shape=[
            jax.ShapeDtypeStruct((rows, width // 2), BF),
            jax.ShapeDtypeStruct((devices, tokens), BF),
        ],
        in_specs=[whole(TOP, tokens), whole(TOP, tokens), whole(tokens, width), whole(tokens, width)],
        out_specs=[pl.BlockSpec((rows // steps, width // 2), lambda g: (g, 0)), whole(devices, tokens)],
        scratch_shapes=[
            pltpu.VMEM((devices, tokens), F32),
            pltpu.VMEM((devices, tokens), F32),
            pltpu.VMEM((4 * tokens, width // 2), BF),
        ],
        compiler_params=pltpu.CompilerParams(vmem_limit_bytes=32 * 2**20),
        cost_estimate=pl.CostEstimate(flops=8 * 10**9, bytes_accessed=8 * 10**6, transcendentals=0),
        name=f"dispatch{which}",
    )(ids_t, w_t, hidden, cot)


def order_in():
    m = np.zeros((192, 192), np.float32)
    for s in range(8):
        for h in range(2):
            for a in range(2):
                for r in range(CAP):
                    m[a * 96 + h * 48 + s * CAP + r, s * 24 + h * 12 + a * CAP + r] = 1
    return m


def order_out():
    m = np.zeros((192, 192), np.float32)
    for s in range(8):
        for q in range(4):
            for r in range(CAP):
                m[s * 24 + q * CAP + r, q * 48 + s * CAP + r] = 1
    return m


def expert_kernel(
    first, rows_ref, into_ref, out_of_ref, gain_ref, gate_ref, up_ref, down_ref, *refs
):
    refs = refs if first else refs[5:]
    send_ref, norm_ref, grad_ref, act_ref, gb_ref, ub_ref, sum_ref, raw_s = refs
    rows = raw_s.shape[0]
    width = raw_s.shape[1]
    half, quarter = width // 2, width // 4
    subs = rows // 48
    for b in range(subs):
        moved = dot(into_ref[...], rows_ref[b * 192 : (b + 1) * 192, :])
        for h in range(2):
            raw_s[b * 48 : (b + 1) * 48, h * half : (h + 1) * half] = moved[h * 48 : (h + 1) * 48, :]
            grad_ref[0, b * 48 : (b + 1) * 48, h * half : (h + 1) * half] = moved[
                96 + h * 48 : 96 + (h + 1) * 48, :
            ].astype(BF)
    raw = raw_s[...]
    root = lax.rsqrt(jnp.mean(raw * raw, axis=1, keepdims=True) + EPSILON)
    scaled = raw * root
    normed = (scaled * gain_ref[...]).astype(BF)
    norm_ref[0] = normed
    pre_gate = dot(normed, gate_ref[0])
    pre_up = dot(normed, up_ref[0])
    sig = jax.nn.sigmoid(pre_gate)
    silu = pre_gate * sig
    act_ref[0] = (silu * pre_up).astype(BF)
    grad_act = dot(grad_ref[0], down_ref[0], 1, 1)
    gate_back = (grad_act * pre_up * sig * (1.0 + pre_gate * (1.0 - sig))).astype(BF)
    up_back = (grad_act * silu).astype(BF)
    gb_ref[0] = gate_back
    ub_ref[0] = up_back
    returned = (dot(gate_back, gate_ref[0], 1, 1) + dot(up_back, up_ref[0], 1, 1)).astype(BF)
    partial = jnp.sum(returned.astype(F32) * (raw_s[...] * root), axis=0, keepdims=True)

    @pl.when(pl.program_id(0) == 0)
    def _():
        sum_ref[...] = jnp.zeros_like(sum_ref)

    sum_ref[...] += partial
    for b in range(subs):
        part = returned[b * 48 : (b + 1) * 48, :]
        stacked = jnp.concatenate([part[:, q * quarter : (q + 1) * quarter] for q in range(4)], axis=0)
        send_ref[b * 192 : (b + 1) * 192, :] = dot(out_of_ref[...], stacked).astype(BF)


def expert(which, arrived, gain, gate, up, down, kept):
    total, half = arrived.shape
    width = 2 * half
    hidden = gate.shape[2]
    experts = gate.shape[0]
    slots = total // 4
    steps = 4
    rows = slots // steps
    whole = lambda *s: pl.BlockSpec(s, lambda g: tuple(0 for _ in s))
    mine = lambda *s: pl.BlockSpec((1, *s), lambda g: (which, 0, 0))
    ours = lambda *s: pl.BlockSpec((1, *s), lambda g: (which, g, 0))
    first = kept is None
    keep_shapes = [(experts, slots, width)] * 2 + [(experts, slots, hidden)] * 3
    keep_specs = [ours(rows, width)] * 2 + [ours(rows, hidden)] * 3
    operands = [
        arrived,
        jnp.asarray(order_in(), BF),
        jnp.asarray(order_out(), BF),
        gain,
        gate,
        up,
        down,
    ]
    in_specs = [
        pl.BlockSpec((rows * 4, half), lambda g: (g, 0)),
        whole(192, 192),
        whole(192, 192),
        whole(1, width),
        mine(width, hidden),
        mine(width, hidden),
        mine(hidden, width),
    ]
    aliases = {}
    if not first:
        aliases = {len(operands) + n: 1 + n for n in range(5)}
        operands += list(kept)
        in_specs += [pl.BlockSpec(memory_space=pl.ANY)] * 5
    outs = pl.pallas_call(
        functools.partial(expert_kernel, first),
        grid=(steps,),
        out_shape=[jax.ShapeDtypeStruct((total, width // 4), BF)]
        + [jax.ShapeDtypeStruct(s, BF) for s in keep_shapes]
        + [jax.ShapeDtypeStruct((1, width), F32)],
        in_specs=in_specs,
        out_specs=[pl.BlockSpec((rows * 4, width // 4), lambda g: (g, 0))] + keep_specs + [whole(1, width)],
        scratch_shapes=[pltpu.VMEM((rows, width), F32)],
        input_output_aliases=aliases,
        compiler_params=pltpu.CompilerParams(vmem_limit_bytes=VMEM_LIMIT),
        cost_estimate=pl.CostEstimate(flops=25 * 10**9, bytes_accessed=22 * 10**6, transcendentals=10**6),
        name=f"expert{which}",
    )(*operands)
    return outs[0], outs[1:6], outs[6]


def combine_kernel(last, tab_ref, rows_ref, slot_ref, part_ref, *refs):
    if last:
        prev_ref, hid_ref, cot_ref, gain_ref, out_ref, acc = refs
    else:
        out_ref, acc = refs
    step = pl.program_id(0)
    count = rows_ref.shape[0]
    group, tokens = tab_ref.shape
    quarter = rows_ref.shape[1]

    @pl.when(step == 0)
    def _():
        acc[...] = jnp.zeros_like(acc)

    at = lax.broadcasted_iota(jnp.int32, (group, count), 1) - 24 * lax.broadcasted_iota(
        jnp.int32, (group, count), 0
    )
    spread = jnp.where((at >= 0) & (at < 24), 1.0, 0.0).astype(BF)
    table = dot(tab_ref[...], spread, 0, 0)
    pick = jnp.where(table == slot_ref[...], 1.0, 0.0)
    left = jnp.concatenate(
        [jnp.where(part_ref[...] == float(q), pick, 0.0).astype(BF) for q in range(4)], axis=0
    )
    acc[...] += dot(left, rows_ref[...])

    @pl.when(step == pl.num_programs(0) - 1)
    def _():
        summed = jnp.concatenate([acc[q * tokens : (q + 1) * tokens, :] for q in range(4)], axis=1)
        if not last:
            out_ref[...] = summed
        else:
            summed = summed + prev_ref[...]
            raw = hid_ref[...].astype(F32)
            root = lax.rsqrt(jnp.mean(raw * raw, axis=1, keepdims=True) + EPSILON)
            scaled = raw * root
            gained = summed * gain_ref[...]
            centre = jnp.mean(gained * scaled, axis=1, keepdims=True)
            out_ref[...] = (cot_ref[...].astype(F32) + root * (gained - scaled * centre)).astype(BF)


def combine(which, table, back, tokens, extra):
    total, quarter = back.shape
    width = 4 * quarter
    devices = table.shape[0]
    steps = 8
    group = devices // steps
    place = np.arange(group * 24) % 24
    slot = jnp.asarray((place % CAP)[None, :], F32)
    part = jnp.asarray((place // CAP)[None, :], F32)
    whole = lambda *s: pl.BlockSpec(s, lambda g: tuple(0 for _ in s))
    last = len(extra) > 0
    extra_specs = [whole(*e.shape) for e in extra]
    return pl.pallas_call(
        functools.partial(combine_kernel, last),
        grid=(steps,),
        out_shape=jax.ShapeDtypeStruct((tokens, width), BF if last else F32),
        in_specs=[
            pl.BlockSpec((group, tokens), lambda g: (g, 0)),
            pl.BlockSpec((group * 24, quarter), lambda g: (g, 0)),
            whole(1, group * 24),
            whole(1, group * 24),
        ]
        + extra_specs,
        out_specs=whole(tokens, width),
        scratch_shapes=[pltpu.VMEM((4 * tokens, quarter), F32)],
        compiler_params=pltpu.CompilerParams(vmem_limit_bytes=32 * 2**20),
        cost_estimate=pl.CostEstimate(flops=4 * 10**9, bytes_accessed=6 * 10**6, transcendentals=0),
        name=f"combine{which}",
    )(table, back, slot, part, *extra)


def exchanged(x, devices):
    rows, columns = x.shape
    out = lax.all_to_all(x.reshape(devices, rows // devices, columns), ("dp", "seq"), 0, 0, tiled=True)
    return out.reshape(rows, columns)


def from_everyone(x, axis):
    peers = lax.axis_size(axis)
    return lax.all_to_all(jnp.broadcast_to(x[None], (peers, *x.shape)), axis, 0, 0, tiled=True)


def shards(
    hidden_in, cotangent, norm_gain, route_weights, expert_ids, expert_gate, expert_up, expert_down
):
    hidden, cot = hidden_in[0], cotangent[0]
    tokens, width = hidden.shape
    devices = lax.axis_size("dp") * lax.axis_size("seq")
    ids_t = expert_ids[0].T
    w_t = route_weights[0].T
    gain = from_everyone(norm_gain, "dp").reshape(1, width)
    sent0, table0 = dispatch(0, devices, ids_t, w_t, hidden, cot)
    sent1, table1 = dispatch(1, devices, ids_t, w_t, hidden, cot)
    came0 = exchanged(sent0, devices)
    came1 = exchanged(sent1, devices)
    ret0, kept, sum0 = expert(0, came0, gain, expert_gate, expert_up, expert_down, None)
    back0 = exchanged(ret0, devices)
    ret1, kept, sum1 = expert(1, came1, gain, expert_gate, expert_up, expert_down, kept)
    back1 = exchanged(ret1, devices)
    normed, grads, act, gate_back, up_back = kept
    outer = lambda a, b: jnp.einsum("era,erb->eab", a, b, preferred_element_type=F32).astype(BF)
    grad_down = outer(act, grads)
    grad_gate = outer(normed, gate_back)
    grad_up = outer(normed, up_back)
    local_gain = (sum0 + sum1).reshape(lax.axis_size("dp"), -1)
    share = jnp.sum(lax.all_to_all(local_gain, "dp", 0, 0, tiled=True), axis=0)
    grad_gain = jnp.sum(from_everyone(share, "seq"), axis=0)
    part0 = combine(0, table0, back0, tokens, ())
    grad_hidden = combine(1, table1, back1, tokens, (part0, hidden, cot, gain))
    return grad_hidden[None], grad_gain, grad_gate, grad_up, grad_down


def solution(mesh):
    rows = P("dp", "seq", None)
    experts = P(("dp", "seq"), None, None)
    return jax.shard_map(
        shards,
        mesh=mesh,
        in_specs=(rows, rows, P("dp"), rows, rows, experts, experts, experts),
        out_specs=(rows, P("dp"), experts, experts, experts),
        check_vma=False,
    )
```

```python
import functools

import jax
import jax.numpy as jnp
import numpy as np
from jax import lax
from jax.experimental import pallas as pl
from jax.experimental.pallas import tpu as pltpu
from jax.sharding import PartitionSpec as P


TOP = 10
EPSILON = 1e-06
CAP = 6
BF = jnp.bfloat16
F32 = jnp.float32
VMEM_LIMIT = 60 * 2**20


def dot(a, b, ca=1, cb=0):
    return lax.dot_general(a, b, (((ca,), (cb,)), ((), ())), preferred_element_type=F32)


def dispatch_kernel(which, ids_ref, w_ref, hid_ref, cot_ref, send_ref, tab_ref, tab_s, wt_s, src_s):
    step = pl.program_id(0)
    tokens = hid_ref.shape[0]
    half = hid_ref.shape[1] // 2
    devices = tab_s.shape[0]

    @pl.when(step == 0)
    def _():
        expert = 2 * lax.broadcasted_iota(jnp.int32, (devices, tokens), 0) + which
        hit = jnp.zeros((devices, tokens), F32)
        weight = jnp.zeros((devices, tokens), F32)
        for k in range(TOP):
            same = ids_ref[k : k + 1, :] == expert
            hit = hit + jnp.where(same, 1.0, 0.0)
            weight = weight + jnp.where(same, w_ref[k : k + 1, :], 0.0)
        earlier = lax.broadcasted_iota(jnp.int32, (tokens, tokens), 0) < lax.broadcasted_iota(
            jnp.int32, (tokens, tokens), 1
        )
        rank = dot(hit.astype(BF), jnp.where(earlier, 1.0, 0.0).astype(BF))
        table = jnp.where(hit > 0.0, rank, -1.0)
        tab_s[...] = table
        tab_ref[...] = table.astype(BF)
        wt_s[...] = weight
        for h in range(2):
            src_s[h * 2 * tokens : h * 2 * tokens + tokens, :] = hid_ref[:, h * half : (h + 1) * half]
            src_s[h * 2 * tokens + tokens : (h + 1) * 2 * tokens, :] = cot_ref[:, h * half : (h + 1) * half]

    group = send_ref.shape[0] // 24
    at = pl.ds(pl.multiple_of(step * group, group), group)
    shape = (group, 24, tokens)
    table = jnp.broadcast_to(tab_s[at, :][:, None, :], shape)
    weight = jnp.broadcast_to(wt_s[at, :][:, None, :], shape)
    row = lax.broadcasted_iota(jnp.int32, shape, 1)
    in_half = jnp.where(row >= 12, 1, 0)
    row = row - 12 * in_half
    is_grad = jnp.where(row >= CAP, 1, 0)
    slot = (row - CAP * is_grad).astype(F32)
    flat = (group * 24, tokens)
    pick = jnp.where(table == slot, 1.0, 0.0)
    scale = jnp.sum(
        jnp.where(is_grad == 1, pick * weight, jnp.where(lax.broadcasted_iota(jnp.int32, shape, 2) == 0, 1.0, 0.0)),
        axis=2,
        keepdims=True,
    ).reshape(flat[0], 1)
    kind = 2 * in_half + is_grad
    pieces = [jnp.where(kind == m, pick, 0.0).reshape(flat).astype(BF) for m in range(4)]
    left = jnp.concatenate(pieces, axis=1)
    send_ref[...] = (dot(left, src_s[...]) * scale).astype(BF)


def dispatch(which, devices, ids_t, w_t, hidden, cot):
    tokens, width = hidden.shape
    steps = 8
    rows = devices * 24
    whole = lambda *s: pl.BlockSpec(s, lambda g: tuple(0 for _ in s))
    return pl.pallas_call(
        functools.partial(dispatch_kernel, which),
        grid=(steps,),
        out_shape=[
            jax.ShapeDtypeStruct((rows, width // 2), BF),
            jax.ShapeDtypeStruct((devices, tokens), BF),
        ],
        in_specs=[whole(TOP, tokens), whole(TOP, tokens), whole(tokens, width), whole(tokens, width)],
        out_specs=[pl.BlockSpec((rows // steps, width // 2), lambda g: (g, 0)), whole(devices, tokens)],
        scratch_shapes=[
            pltpu.VMEM((devices, tokens), F32),
            pltpu.VMEM((devices, tokens), F32),
            pltpu.VMEM((4 * tokens, width // 2), BF),
        ],
        compiler_params=pltpu.CompilerParams(vmem_limit_bytes=32 * 2**20),
        cost_estimate=pl.CostEstimate(flops=8 * 10**9, bytes_accessed=8 * 10**6, transcendentals=0),
    )(ids_t, w_t, hidden, cot)


def order_in():
    m = np.zeros((192, 192), np.float32)
    for s in range(8):
        for h in range(2):
            for a in range(2):
                for r in range(CAP):
                    m[a * 96 + h * 48 + s * CAP + r, s * 24 + h * 12 + a * CAP + r] = 1
    return m


def order_out():
    m = np.zeros((192, 192), np.float32)
    for s in range(8):
        for q in range(4):
            for r in range(CAP):
                m[s * 24 + q * CAP + r, q * 48 + s * CAP + r] = 1
    return m


def expert_kernel(
    first, rows_ref, into_ref, out_of_ref, gain_ref, gate_ref, up_ref, down_ref, *refs
):
    refs = refs if first else refs[5:]
    send_ref, norm_ref, grad_ref, act_ref, gb_ref, ub_ref, sum_ref, raw_s = refs
    rows = raw_s.shape[0]
    width = raw_s.shape[1]
    half, quarter = width // 2, width // 4
    subs = rows // 48
    for b in range(subs):
        moved = dot(into_ref[...], rows_ref[b * 192 : (b + 1) * 192, :])
        for h in range(2):
            raw_s[b * 48 : (b + 1) * 48, h * half : (h + 1) * half] = moved[h * 48 : (h + 1) * 48, :]
            grad_ref[0, b * 48 : (b + 1) * 48, h * half : (h + 1) * half] = moved[
                96 + h * 48 : 96 + (h + 1) * 48, :
            ].astype(BF)
    raw = raw_s[...]
    root = lax.rsqrt(jnp.mean(raw * raw, axis=1, keepdims=True) + EPSILON)
    scaled = raw * root
    normed = (scaled * gain_ref[...]).astype(BF)
    norm_ref[0] = normed
    pre_gate = dot(normed, gate_ref[0])
    pre_up = dot(normed, up_ref[0])
    sig = jax.nn.sigmoid(pre_gate)
    silu = pre_gate * sig
    act_ref[0] = (silu * pre_up).astype(BF)
    grad_act = dot(grad_ref[0], down_ref[0], 1, 1)
    gate_back = (grad_act * pre_up * sig * (1.0 + pre_gate * (1.0 - sig))).astype(BF)
    up_back = (grad_act * silu).astype(BF)
    gb_ref[0] = gate_back
    ub_ref[0] = up_back
    returned = (dot(gate_back, gate_ref[0], 1, 1) + dot(up_back, up_ref[0], 1, 1)).astype(BF)
    partial = jnp.sum(returned.astype(F32) * (raw_s[...] * root), axis=0, keepdims=True)

    @pl.when(pl.program_id(0) == 0)
    def _():
        sum_ref[...] = jnp.zeros_like(sum_ref)

    sum_ref[...] += partial
    for b in range(subs):
        part = returned[b * 48 : (b + 1) * 48, :]
        stacked = jnp.concatenate([part[:, q * quarter : (q + 1) * quarter] for q in range(4)], axis=0)
        send_ref[b * 192 : (b + 1) * 192, :] = dot(out_of_ref[...], stacked).astype(BF)


def expert(which, arrived, gain, gate, up, down, kept):
    total, half = arrived.shape
    width = 2 * half
    hidden = gate.shape[2]
    experts = gate.shape[0]
    slots = total // 4
    steps = 4
    rows = slots // steps
    whole = lambda *s: pl.BlockSpec(s, lambda g: tuple(0 for _ in s))
    mine = lambda *s: pl.BlockSpec((1, *s), lambda g: (which, 0, 0))
    ours = lambda *s: pl.BlockSpec((1, *s), lambda g: (which, g, 0))
    first = kept is None
    keep_shapes = [(experts, slots, width)] * 2 + [(experts, slots, hidden)] * 3
    keep_specs = [ours(rows, width)] * 2 + [ours(rows, hidden)] * 3
    operands = [
        arrived,
        jnp.asarray(order_in(), BF),
        jnp.asarray(order_out(), BF),
        gain,
        gate,
        up,
        down,
    ]
    in_specs = [
        pl.BlockSpec((rows * 4, half), lambda g: (g, 0)),
        whole(192, 192),
        whole(192, 192),
        whole(1, width),
        mine(width, hidden),
        mine(width, hidden),
        mine(hidden, width),
    ]
    aliases = {}
    if not first:
        aliases = {len(operands) + n: 1 + n for n in range(5)}
        operands += list(kept)
        in_specs += [pl.BlockSpec(memory_space=pl.ANY)] * 5
    outs = pl.pallas_call(
        functools.partial(expert_kernel, first),
        grid=(steps,),
        out_shape=[jax.ShapeDtypeStruct((total, width // 4), BF)]
        + [jax.ShapeDtypeStruct(s, BF) for s in keep_shapes]
        + [jax.ShapeDtypeStruct((1, width), F32)],
        in_specs=in_specs,
        out_specs=[pl.BlockSpec((rows * 4, width // 4), lambda g: (g, 0))] + keep_specs + [whole(1, width)],
        scratch_shapes=[pltpu.VMEM((rows, width), F32)],
        input_output_aliases=aliases,
        compiler_params=pltpu.CompilerParams(vmem_limit_bytes=VMEM_LIMIT),
        cost_estimate=pl.CostEstimate(flops=25 * 10**9, bytes_accessed=22 * 10**6, transcendentals=10**6),
    )(*operands)
    return outs[0], outs[1:6], outs[6]


def combine_kernel(last, tab_ref, rows_ref, slot_ref, part_ref, *refs):
    if last:
        prev_ref, hid_ref, cot_ref, gain_ref, out_ref, acc = refs
    else:
        out_ref, acc = refs
    step = pl.program_id(0)
    count = rows_ref.shape[0]
    group, tokens = tab_ref.shape

    @pl.when(step == 0)
    def _():
        acc[...] = jnp.zeros_like(acc)

    at = lax.broadcasted_iota(jnp.int32, (group, count), 1) - 24 * lax.broadcasted_iota(
        jnp.int32, (group, count), 0
    )
    spread = jnp.where((at >= 0) & (at < 24), 1.0, 0.0).astype(BF)
    table = dot(tab_ref[...], spread, 0, 0)
    pick = jnp.where(table == slot_ref[...], 1.0, 0.0)
    left = jnp.concatenate(
        [jnp.where(part_ref[...] == float(q), pick, 0.0).astype(BF) for q in range(4)], axis=0
    )
    acc[...] += dot(left, rows_ref[...])

    @pl.when(step == pl.num_programs(0) - 1)
    def _():
        summed = jnp.concatenate([acc[q * tokens : (q + 1) * tokens, :] for q in range(4)], axis=1)
        if not last:
            out_ref[...] = summed
        else:
            summed = summed + prev_ref[...]
            raw = hid_ref[...].astype(F32)
            root = lax.rsqrt(jnp.mean(raw * raw, axis=1, keepdims=True) + EPSILON)
            scaled = raw * root
            gained = summed * gain_ref[...]
            centre = jnp.mean(gained * scaled, axis=1, keepdims=True)
            out_ref[...] = (cot_ref[...].astype(F32) + root * (gained - scaled * centre)).astype(BF)


def combine(table, back, tokens, extra):
    _, quarter = back.shape
    width = 4 * quarter
    devices = table.shape[0]
    steps = 8
    group = devices // steps
    place = np.arange(group * 24) % 24
    slot = jnp.asarray((place % CAP)[None, :], F32)
    part = jnp.asarray((place // CAP)[None, :], F32)
    whole = lambda *s: pl.BlockSpec(s, lambda g: tuple(0 for _ in s))
    last = len(extra) > 0
    extra_specs = [whole(*e.shape) for e in extra]
    return pl.pallas_call(
        functools.partial(combine_kernel, last),
        grid=(steps,),
        out_shape=jax.ShapeDtypeStruct((tokens, width), BF if last else F32),
        in_specs=[
            pl.BlockSpec((group, tokens), lambda g: (g, 0)),
            pl.BlockSpec((group * 24, quarter), lambda g: (g, 0)),
            whole(1, group * 24),
            whole(1, group * 24),
        ]
        + extra_specs,
        out_specs=whole(tokens, width),
        scratch_shapes=[pltpu.VMEM((4 * tokens, quarter), F32)],
        compiler_params=pltpu.CompilerParams(vmem_limit_bytes=32 * 2**20),
        cost_estimate=pl.CostEstimate(flops=4 * 10**9, bytes_accessed=6 * 10**6, transcendentals=0),
    )(table, back, slot, part, *extra)


def exchanged(x, devices):
    rows, columns = x.shape
    out = lax.all_to_all(x.reshape(devices, rows // devices, columns), ("dp", "seq"), 0, 0, tiled=True)
    return out.reshape(rows, columns)


def shards(
    hidden_in, cotangent, norm_gain, route_weights, expert_ids, expert_gate, expert_up, expert_down
):
    hidden, cot = hidden_in[0], cotangent[0]
    tokens, width = hidden.shape
    devices = lax.axis_size("dp") * lax.axis_size("seq")
    ids_t = expert_ids[0].T
    w_t = route_weights[0].T
    gain = lax.all_gather(norm_gain, "dp", tiled=True).reshape(1, width)
    sent0, table0 = dispatch(0, devices, ids_t, w_t, hidden, cot)
    came0 = exchanged(sent0, devices)
    sent1, table1 = dispatch(1, devices, ids_t, w_t, hidden, cot)
    came1 = exchanged(sent1, devices)
    ret0, kept, sum0 = expert(0, came0, gain, expert_gate, expert_up, expert_down, None)
    back0 = exchanged(ret0, devices)
    ret1, kept, sum1 = expert(1, came1, gain, expert_gate, expert_up, expert_down, kept)
    back1 = exchanged(ret1, devices)
    normed, grads, act, gate_back, up_back = kept
    outer = lambda a, b: jnp.einsum("era,erb->eab", a, b, preferred_element_type=F32).astype(BF)
    grad_down = outer(act, grads)
    grad_gate = outer(normed, gate_back)
    grad_up = outer(normed, up_back)
    everyone = lax.psum((sum0 + sum1).reshape(-1), ("dp", "seq"))
    share = width // lax.axis_size("dp")
    grad_gain = lax.dynamic_slice(everyone, (lax.axis_index("dp") * share,), (share,))
    part0 = combine(table0, back0, tokens, ())
    grad_hidden = combine(table1, back1, tokens, (part0, hidden, cot, gain))
    return grad_hidden[None], grad_gain, grad_gate, grad_up, grad_down


def solution(mesh):
    rows = P("dp", "seq", None)
    experts = P(("dp", "seq"), None, None)
    return jax.shard_map(
        shards,
        mesh=mesh,
        in_specs=(rows, rows, P("dp"), rows, rows, experts, experts, experts),
        out_specs=(rows, P("dp"), experts, experts, experts),
        check_vma=False,
    )
```

```python
import jax
import jax.numpy as jnp
import numpy as np
from jax import lax
from jax.experimental import pallas as pl
from jax.experimental.pallas import tpu as pltpu
from jax.sharding import PartitionSpec as P

TOP = 10
EPSILON = 1e-06
CAP = 6
BF = jnp.bfloat16
F32 = jnp.float32
VMEM_LIMIT = 62 * 2**20
MESH = pl.DeviceIdType.MESH
STRIDE = 37


def dot(a, b, ca=1, cb=0):
    return lax.dot_general(a, b, (((ca,), (cb,)), ((), ())), preferred_element_type=F32)


def dispatch_kernel(ids_ref, w_ref, dest_ref, hid_ref, cot_ref, send_ref, tab_ref, tab_s, wt_s, src_s):
    which, step = pl.program_id(0), pl.program_id(1)
    tokens = hid_ref.shape[0]
    half = hid_ref.shape[1] // 2
    devices = tab_s.shape[0]

    @pl.when((which == 0) & (step == 0))
    def _():
        for h in range(2):
            src_s[h * 2 * tokens : h * 2 * tokens + tokens, :] = hid_ref[:, h * half : (h + 1) * half]
            src_s[h * 2 * tokens + tokens : (h + 1) * 2 * tokens, :] = cot_ref[:, h * half : (h + 1) * half]

    @pl.when(step == 0)
    def _():
        expert = jnp.broadcast_to(2 * dest_ref[...] + which, (devices, tokens))
        hit = jnp.zeros((devices, tokens), F32)
        weight = jnp.zeros((devices, tokens), F32)
        for k in range(TOP):
            same = ids_ref[k : k + 1, :] == expert
            hit = hit + jnp.where(same, 1.0, 0.0)
            weight = weight + jnp.where(same, w_ref[k : k + 1, :], 0.0)
        earlier = lax.broadcasted_iota(jnp.int32, (tokens, tokens), 0) < lax.broadcasted_iota(
            jnp.int32, (tokens, tokens), 1
        )
        rank = dot(hit.astype(BF), jnp.where(earlier, 1.0, 0.0).astype(BF))
        table = jnp.where(hit > 0.0, rank, -1.0)
        tab_s[...] = table
        tab_ref[0] = table.astype(BF)
        wt_s[...] = weight

    group = send_ref.shape[1] // 24
    at = pl.ds(pl.multiple_of(step * group, group), group)
    shape = (group, 24, tokens)
    table = jnp.broadcast_to(tab_s[at, :][:, None, :], shape)
    weight = jnp.broadcast_to(wt_s[at, :][:, None, :], shape)
    row = lax.broadcasted_iota(jnp.int32, shape, 1)
    in_half = jnp.where(row >= 12, 1, 0)
    row = row - 12 * in_half
    is_grad = jnp.where(row >= CAP, 1, 0)
    slot = (row - CAP * is_grad).astype(F32)
    flat = (group * 24, tokens)
    pick = jnp.where(table == slot, 1.0, 0.0)
    scale = jnp.sum(
        jnp.where(is_grad == 1, pick * weight, jnp.where(lax.broadcasted_iota(jnp.int32, shape, 2) == 0, 1.0, 0.0)),
        axis=2,
        keepdims=True,
    ).reshape(flat[0], 1)
    kind = 2 * in_half + is_grad
    pieces = [jnp.where(kind == m, pick, 0.0).reshape(flat).astype(BF) for m in range(4)]
    left = jnp.concatenate(pieces, axis=1)
    send_ref[0] = (dot(left, src_s[...]) * scale).astype(BF)


def dispatch(devices, ids_t, w_t, dest, hidden, cot):
    tokens, width = hidden.shape
    steps = 8
    rows = devices * 24
    whole = lambda *s: pl.BlockSpec(s, lambda i, g: tuple(0 for _ in s))
    return pl.pallas_call(
        dispatch_kernel,
        grid=(2, steps),
        out_shape=[
            jax.ShapeDtypeStruct((2, rows, width // 2), BF),
            jax.ShapeDtypeStruct((2, devices, tokens), BF),
        ],
        in_specs=[
            whole(TOP, tokens),
            whole(TOP, tokens),
            whole(devices, 1),
            whole(tokens, width),
            whole(tokens, width),
        ],
        out_specs=[
            pl.BlockSpec((1, rows // steps, width // 2), lambda i, g: (i, g, 0)),
            pl.BlockSpec((1, devices, tokens), lambda i, g: (i, 0, 0)),
        ],
        scratch_shapes=[
            pltpu.VMEM((devices, tokens), F32),
            pltpu.VMEM((devices, tokens), F32),
            pltpu.VMEM((4 * tokens, width // 2), BF),
        ],
        compiler_params=pltpu.CompilerParams(vmem_limit_bytes=32 * 2**20),
        cost_estimate=pl.CostEstimate(flops=8 * 10**9, bytes_accessed=16 * 10**6, transcendentals=0),
        name="dispatch",
    )(ids_t, w_t, dest, hidden, cot)


def order_in():
    m = np.zeros((192, 192), np.float32)
    for s in range(8):
        for h in range(2):
            for a in range(2):
                for r in range(CAP):
                    m[a * 96 + h * 48 + s * CAP + r, s * 24 + h * 12 + a * CAP + r] = 1
    return m


def order_out():
    m = np.zeros((192, 192), np.float32)
    for s in range(8):
        for q in range(4):
            for r in range(CAP):
                m[s * 24 + q * CAP + r, q * 48 + s * CAP + r] = 1
    return m


def place(n):
    v = ((n + 1) * STRIDE) % 128
    return v // 32, (v // 8) % 4, (v // 2) % 4, v % 2


def here():
    dp, seq = lax.axis_index("dp"), lax.axis_index("seq")
    return dp % 4, dp // 4, seq // 2, seq % 2


def device_at(n, sign):
    x, y, z, core = here()
    dx, dy, dz, dcore = place(n)
    x, y, z = (x + sign * dx + 4) % 4, (y + sign * dy + 4) % 4, (z + sign * dz + 4) % 4
    return y * 4 + x, z * 2 + (core + dcore) % 2


def core_kernel(
    send, gain_in, gate, up, down, into_ref, out_of_ref,
    back, ret, came, total_ref, gain_ref, d_gate, d_up, d_down,
    gain_s, g_gate, g_up, g_down, raw_s, rows_s, norm_s, grad_s, act_s, gb_s, ub_s, ret_s, dw_s, dd_s,
    sum_s, piece_s, arrive_s, share_s, share_in_s,
    w_sem, gain_send, gain_recv, f_send, f_recv, r_send, r_recv, load_sem, store_sem, dw_sem, t_send, t_recv,
):
    dp, seq = lax.axis_index("dp"), lax.axis_index("seq")
    devices = 128
    width = norm_s.shape[2]
    half, quarter = width // 2, width // 4
    group = 32
    rows = group * CAP

    def gain_copy(i):
        return pltpu.make_async_remote_copy(
            gain_in, gain_s.at[dp], gain_send, gain_recv, device_id=((dp + i) % 16, seq), device_id_type=MESH
        )

    own_gain = pltpu.make_async_copy(gain_in, gain_s.at[dp], gain_recv)
    own_gain.start()

    @pl.loop(1, 16)
    def _(i):
        gain_copy(i).start()

    def at(n, size=1):
        return pl.ds(pl.multiple_of(n * 24, 8), size * 24)

    for w in range(2):
        @pl.loop(0, devices - 1)
        def _(n):
            pltpu.make_async_remote_copy(
                send.at[w, at(n)],
                came.at[w, at(n)],
                f_send.at[w],
                f_recv.at[w * 4 + n // group],
                device_id=device_at(n, 1),
                device_id_type=MESH,
            ).start()

        pltpu.make_async_copy(send.at[w, at(devices - 1)], came.at[w, at(devices - 1)], f_recv.at[w * 4 + 3]).start()

    loads = [
        pltpu.make_async_copy(gate, g_gate, w_sem.at[0]),
        pltpu.make_async_copy(up, g_up, w_sem.at[1]),
        pltpu.make_async_copy(down, g_down, w_sem.at[2]),
    ]
    for c in loads:
        c.start()
    for c in loads:
        c.wait()
    pltpu.make_async_copy(gain_s, gain_s, gain_recv).wait()
    gain_ref[...] = jnp.concatenate([gain_s[i] for i in range(16)], axis=1)
    sum_s[...] = jnp.zeros_like(sum_s)

    @pl.loop(0, 8)
    def _(step):
        w, g = step // 4, step % 4
        slab = at(g * group, group)
        pltpu.make_async_copy(came.at[w, slab], came.at[w, slab], f_recv.at[step]).wait()
        load = pltpu.make_async_copy(came.at[w, slab], rows_s, load_sem)
        load.start()
        load.wait()
        mine = pl.ds(pl.multiple_of(g * rows, rows), rows)
        for b in range(4):
            moved = dot(into_ref[...], rows_s[b * 192 : (b + 1) * 192, :])
            there = pl.ds(pl.multiple_of(g * rows + b * 48, 16), 48)
            for h in range(2):
                raw_s[b * 48 : (b + 1) * 48, h * half : (h + 1) * half] = moved[h * 48 : (h + 1) * 48, :]
                grad_s[w, there, h * half : (h + 1) * half] = moved[96 + h * 48 : 96 + (h + 1) * 48, :].astype(BF)
        raw = raw_s[...]
        root = lax.rsqrt(jnp.mean(raw * raw, axis=1, keepdims=True) + EPSILON)
        normed = (raw * root * gain_ref[...]).astype(BF)
        norm_s[w, mine, :] = normed
        pre_gate = dot(normed, g_gate[w])
        pre_up = dot(normed, g_up[w])
        sig = jax.nn.sigmoid(pre_gate)
        silu = pre_gate * sig
        act_s[w, mine, :] = (silu * pre_up).astype(BF)
        grad_act = dot(grad_s[w, mine, :], g_down[w], 1, 1)
        gate_back = (grad_act * pre_up * sig * (1.0 + pre_gate * (1.0 - sig))).astype(BF)
        up_back = (grad_act * silu).astype(BF)
        gb_s[w, mine, :] = gate_back
        ub_s[w, mine, :] = up_back
        returned = (dot(gate_back, g_gate[w], 1, 1) + dot(up_back, g_up[w], 1, 1)).astype(BF)
        sum_s[...] += jnp.sum(returned.astype(F32) * (raw_s[...] * root), axis=0, keepdims=True)
        for b in range(4):
            part = returned[b * 48 : (b + 1) * 48, :]
            stacked = jnp.concatenate([part[:, q * quarter : (q + 1) * quarter] for q in range(4)], axis=0)
            ret_s[b * 192 : (b + 1) * 192, :] = dot(out_of_ref[...], stacked).astype(BF)
        store = pltpu.make_async_copy(ret_s, ret.at[w, slab], store_sem)
        store.start()
        store.wait()

        @pl.loop(g * group, jnp.minimum(g * group + group, devices - 1))
        def _(n):
            pltpu.make_async_remote_copy(
                ret.at[w, at(n)],
                back.at[w, at(n)],
                r_send,
                r_recv.at[w],
                device_id=device_at(n, -1),
                device_id_type=MESH,
            ).start()

    for w in range(2):
        last = at(devices - 1)
        pltpu.make_async_copy(ret.at[w, last], back.at[w, last], r_recv.at[w]).start()

    for p in range(16):
        piece_s[p] = sum_s[:, p * 128 : (p + 1) * 128]

    def piece(i):
        return pltpu.make_async_remote_copy(
            piece_s.at[(dp + i) % 16], arrive_s.at[i], t_send.at[0], t_recv.at[0],
            device_id=((dp + i) % 16, seq), device_id_type=MESH,
        )

    @pl.loop(1, 16)
    def _(i):
        piece(i).start()

    block = 256
    for w in range(2):
        if w == 1:
            for c in stores:
                c.wait()

        @pl.loop(0, width // block)
        def _(j):
            lanes = pl.ds(pl.multiple_of(j * block, block), block)
            left = norm_s[w, :, lanes]
            dw_s[0, lanes, :] = dot(left, gb_s[w], 0, 0).astype(BF)
            dw_s[1, lanes, :] = dot(left, ub_s[w], 0, 0).astype(BF)
            dd_s[:, lanes] = dot(act_s[w], grad_s[w, :, lanes], 0, 0).astype(BF)

        stores = [
            pltpu.make_async_copy(dw_s.at[0], d_gate.at[w], dw_sem.at[0]),
            pltpu.make_async_copy(dw_s.at[1], d_up.at[w], dw_sem.at[1]),
            pltpu.make_async_copy(dd_s, d_down.at[w], dw_sem.at[2]),
        ]
        for c in stores:
            c.start()

    fifteen = arrive_s.at[pl.ds(1, 15)]
    pltpu.make_async_copy(fifteen, fifteen, t_recv.at[0]).wait()
    share = piece_s[dp]
    for i in range(1, 16):
        share = share + arrive_s[i]
    share_s[...] = share

    def to_copy(i):
        return pltpu.make_async_remote_copy(
            share_s, share_in_s.at[i], t_send.at[1], t_recv.at[1], device_id=(dp, (seq + i) % 8), device_id_type=MESH
        )

    @pl.loop(1, 8)
    def _(i):
        to_copy(i).start()

    for c in stores:
        c.wait()
    for w in range(2):
        pltpu.make_async_copy(back.at[w], back.at[w], r_recv.at[w]).wait()
    seven = share_in_s.at[pl.ds(1, 7)]
    pltpu.make_async_copy(seven, seven, t_recv.at[1]).wait()
    for i in range(1, 8):
        share = share + share_in_s[i]
    total_ref[...] = share

    most = at(0, devices - 1)
    for w in range(2):
        pltpu.make_async_copy(send.at[w, most], send.at[w, most], f_send.at[w]).wait()
        pltpu.make_async_copy(ret.at[w, most], ret.at[w, most], r_send).wait()
    pltpu.make_async_copy(fifteen, fifteen, t_send.at[0]).wait()
    pltpu.make_async_copy(seven, seven, t_send.at[1]).wait()
    pltpu.make_async_copy(gain_s.at[pl.ds(1, 15)], gain_s.at[pl.ds(1, 15)], gain_send).wait()


def core(send, gain, gate, up, down):
    _, total, half = send.shape
    width = 2 * half
    experts, _, hidden = gate.shape
    slots = total // 4
    hbm = pl.BlockSpec(memory_space=pl.ANY)
    vmem = pl.BlockSpec(memory_space=pltpu.VMEM)
    back = jax.ShapeDtypeStruct((2, total, width // 4), BF)
    dma = pltpu.SemaphoreType.DMA
    outs = pl.pallas_call(
        core_kernel,
        out_shape=[
            back,
            back,
            jax.ShapeDtypeStruct(send.shape, BF),
            jax.ShapeDtypeStruct((1, 128), F32),
            jax.ShapeDtypeStruct((1, width), F32),
            jax.ShapeDtypeStruct(gate.shape, BF),
            jax.ShapeDtypeStruct(up.shape, BF),
            jax.ShapeDtypeStruct(down.shape, BF),
        ],
        in_specs=[hbm] * 5 + [vmem] * 2,
        out_specs=[hbm] * 3 + [vmem] * 2 + [hbm] * 3,
        scratch_shapes=[
            pltpu.VMEM((16, 1, 128), F32),
            pltpu.VMEM(gate.shape, BF),
            pltpu.VMEM(up.shape, BF),
            pltpu.VMEM(down.shape, BF),
            pltpu.VMEM((slots // 4, width), F32),
            pltpu.VMEM((total // 4, half), BF),
            pltpu.VMEM((experts, slots, width), BF),
            pltpu.VMEM((experts, slots, width), BF),
            pltpu.VMEM((experts, slots, hidden), BF),
            pltpu.VMEM((experts, slots, hidden), BF),
            pltpu.VMEM((experts, slots, hidden), BF),
            pltpu.VMEM((total // 4, width // 4), BF),
            pltpu.VMEM((2, width, hidden), BF),
            pltpu.VMEM((hidden, width), BF),
            pltpu.VMEM((1, width), F32),
            pltpu.VMEM((16, 1, 128), F32),
            pltpu.VMEM((16, 1, 128), F32),
            pltpu.VMEM((1, 128), F32),
            pltpu.VMEM((8, 1, 128), F32),
            dma((3,)), dma, dma, dma((2,)), dma((8,)), dma, dma((2,)), dma, dma, dma((3,)), dma((2,)), dma((2,)),
        ],
        compiler_params=pltpu.CompilerParams(has_side_effects=True, vmem_limit_bytes=VMEM_LIMIT),
        cost_estimate=pl.CostEstimate(flops=40 * 10**9, bytes_accessed=80 * 10**6, transcendentals=10**6),
        name="core",
    )(send, gain, gate, up, down, jnp.asarray(order_in(), BF), jnp.asarray(order_out(), BF))
    return outs[0], outs[3], outs[4], outs[5], outs[6], outs[7]


def combine_kernel(tab_ref, rows_ref, slot_ref, part_ref, hid_ref, cot_ref, gain_ref, out_ref, acc):
    step = pl.program_id(0) * pl.num_programs(1) + pl.program_id(1)
    count = rows_ref.shape[1]
    group, tokens = tab_ref.shape[1:]

    @pl.when(step == 0)
    def _():
        acc[...] = jnp.zeros_like(acc)

    at = lax.broadcasted_iota(jnp.int32, (group, count), 1) - 24 * lax.broadcasted_iota(
        jnp.int32, (group, count), 0
    )
    spread = jnp.where((at >= 0) & (at < 24), 1.0, 0.0).astype(BF)
    table = dot(tab_ref[0], spread, 0, 0)
    pick = jnp.where(table == slot_ref[...], 1.0, 0.0)
    left = jnp.concatenate(
        [jnp.where(part_ref[...] == float(q), pick, 0.0).astype(BF) for q in range(4)], axis=0
    )
    acc[...] += dot(left, rows_ref[0])

    @pl.when(step == pl.num_programs(0) * pl.num_programs(1) - 1)
    def _():
        summed = jnp.concatenate([acc[q * tokens : (q + 1) * tokens, :] for q in range(4)], axis=1)
        raw = hid_ref[...].astype(F32)
        root = lax.rsqrt(jnp.mean(raw * raw, axis=1, keepdims=True) + EPSILON)
        scaled = raw * root
        gained = summed * gain_ref[...]
        centre = jnp.mean(gained * scaled, axis=1, keepdims=True)
        out_ref[...] = (cot_ref[...].astype(F32) + root * (gained - scaled * centre)).astype(BF)


def combine(table, back, tokens, hidden, cot, gain):
    _, total, quarter = back.shape
    width = 4 * quarter
    devices = table.shape[1]
    steps = 8
    group = devices // steps
    place_in = np.arange(group * 24) % 24
    slot = jnp.asarray((place_in % CAP)[None, :], F32)
    part = jnp.asarray((place_in // CAP)[None, :], F32)
    whole = lambda *s: pl.BlockSpec(s, lambda i, g: tuple(0 for _ in s))
    return pl.pallas_call(
        combine_kernel,
        grid=(2, steps),
        out_shape=jax.ShapeDtypeStruct((tokens, width), BF),
        in_specs=[
            pl.BlockSpec((1, group, tokens), lambda i, g: (i, g, 0)),
            pl.BlockSpec((1, group * 24, quarter), lambda i, g: (i, g, 0)),
            whole(1, group * 24),
            whole(1, group * 24),
            whole(tokens, width),
            whole(tokens, width),
            whole(1, width),
        ],
        out_specs=whole(tokens, width),
        scratch_shapes=[pltpu.VMEM((4 * tokens, quarter), F32)],
        compiler_params=pltpu.CompilerParams(vmem_limit_bytes=32 * 2**20),
        cost_estimate=pl.CostEstimate(flops=8 * 10**9, bytes_accessed=10 * 10**6, transcendentals=0),
        name="combine",
    )(table, back, slot, part, hidden, cot, gain)


def shards(
    hidden_in, cotangent, norm_gain, route_weights, expert_ids, expert_gate, expert_up, expert_down
):
    hidden, cot = hidden_in[0], cotangent[0]
    tokens, width = hidden.shape
    devices = lax.axis_size("dp") * lax.axis_size("seq")
    ids_t = expert_ids[0].T
    w_t = route_weights[0].T
    dp, seq = device_at(jnp.arange(devices, dtype=jnp.int32), 1)
    dest = (dp * 8 + seq).astype(jnp.int32).reshape(devices, 1)
    send, table = dispatch(devices, ids_t, w_t, dest, hidden, cot)
    back, grad_gain, gain, grad_gate, grad_up, grad_down = core(
        send, norm_gain.reshape(1, -1), expert_gate, expert_up, expert_down
    )
    grad_hidden = combine(table, back, tokens, hidden, cot, gain)
    return grad_hidden[None], grad_gain.reshape(-1), grad_gate, grad_up, grad_down


def solution(mesh):
    rows = P("dp", "seq", None)
    experts = P(("dp", "seq"), None, None)
    return jax.shard_map(
        shards,
        mesh=mesh,
        in_specs=(rows, rows, P("dp"), rows, rows, experts, experts, experts),
        out_specs=(rows, P("dp"), experts, experts, experts),
        check_vma=False,
    )
```

```python
import jax
import jax.numpy as jnp
import numpy as np
from jax import lax
from jax.experimental import pallas as pl
from jax.experimental.pallas import tpu as pltpu
from jax.sharding import PartitionSpec as P

TOP = 10
EPSILON = 1e-06
CAP = 6
BF = jnp.bfloat16
F32 = jnp.float32
VMEM_LIMIT = 62 * 2**20
MESH = pl.DeviceIdType.MESH
STRIDE = 37


def dot(a, b, ca=1, cb=0):
    return lax.dot_general(a, b, (((ca,), (cb,)), ((), ())), preferred_element_type=F32)


def order_in():
    m = np.zeros((192, 192), np.float32)
    for s in range(8):
        for h in range(2):
            for a in range(2):
                for r in range(CAP):
                    m[a * 96 + h * 48 + s * CAP + r, s * 24 + h * 12 + a * CAP + r] = 1
    return m


def order_out():
    m = np.zeros((192, 192), np.float32)
    for s in range(8):
        for q in range(4):
            for r in range(CAP):
                m[s * 24 + q * CAP + r, q * 48 + s * CAP + r] = 1
    return m


def place(n):
    v = ((n + 1) * STRIDE) % 128
    return v // 32, (v // 8) % 4, (v // 2) % 4, v % 2


def here():
    dp, seq = lax.axis_index("dp"), lax.axis_index("seq")
    return dp % 4, dp // 4, seq // 2, seq % 2


def device_at(n, sign):
    x, y, z, core = here()
    dx, dy, dz, dcore = place(n)
    x, y, z = (x + sign * dx + 4) % 4, (y + sign * dy + 4) % 4, (z + sign * dz + 4) % 4
    return y * 4 + x, z * 2 + (core + dcore) % 2


def core_kernel(
    ids_ref, w_ref, dest_ref, hid_ref, cot_ref, gain_in, gate, up, down, into_ref, out_of_ref, slot_ref, part_ref,
    hidden_ref, total_ref, back, ret, came, send, d_gate, d_up, d_down,
    tab_s, wt_s, src_s, pack_s, back_s, sum_s, gain_ref, gain_s, g_gate, g_up, g_down, raw_s, rows_s, norm_s, grad_s, act_s, gb_s, ub_s, ret_s, dw_s, dd_s,
    gsum_s, piece_s, arrive_s, share_s, share_in_s,
    pack_sem, w_sem, gain_send, gain_recv, f_send, f_recv, r_send, r_recv, load_sem, store_sem, dw_sem, t_send, t_recv,
):
    dp, seq = lax.axis_index("dp"), lax.axis_index("seq")
    devices = 128
    width = norm_s.shape[2]
    half, quarter = width // 2, width // 4
    group = 32
    rows = group * CAP

    def gain_copy(i):
        return pltpu.make_async_remote_copy(
            gain_in, gain_s.at[dp], gain_send, gain_recv, device_id=((dp + i) % 16, seq), device_id_type=MESH
        )

    own_gain = pltpu.make_async_copy(gain_in, gain_s.at[dp], gain_recv)
    own_gain.start()

    @pl.loop(1, 16)
    def _(i):
        gain_copy(i).start()

    loads = [
        pltpu.make_async_copy(gate, g_gate, w_sem.at[0]),
        pltpu.make_async_copy(up, g_up, w_sem.at[1]),
        pltpu.make_async_copy(down, g_down, w_sem.at[2]),
    ]
    for c in loads:
        c.start()

    def at(n, size=1):
        return pl.ds(pl.multiple_of(n * 24, 8), size * 24)

    tokens = hid_ref.shape[0]
    for h in range(2):
        src_s[h * 2 * tokens : h * 2 * tokens + tokens, :] = hid_ref[:, h * half : (h + 1) * half]
        src_s[h * 2 * tokens + tokens : (h + 1) * 2 * tokens, :] = cot_ref[:, h * half : (h + 1) * half]
    earlier = lax.broadcasted_iota(jnp.int32, (tokens, tokens), 0) < lax.broadcasted_iota(
        jnp.int32, (tokens, tokens), 1
    )
    before = jnp.where(earlier, 1.0, 0.0).astype(BF)
    for w in range(2):
        expert = jnp.broadcast_to(2 * dest_ref[...] + w, (devices, tokens))
        hit = jnp.zeros((devices, tokens), F32)
        weight = jnp.zeros((devices, tokens), F32)
        for k in range(TOP):
            same = ids_ref[k : k + 1, :] == expert
            hit = hit + jnp.where(same, 1.0, 0.0)
            weight = weight + jnp.where(same, w_ref[k : k + 1, :], 0.0)
        tab_s[w] = jnp.where(hit > 0.0, dot(hit.astype(BF), before), -1.0)
        wt_s[w] = weight

    block = 16
    shape = (block, 24, tokens)
    row = lax.broadcasted_iota(jnp.int32, shape, 1)
    in_half = jnp.where(row >= 12, 1, 0)
    row = row - 12 * in_half
    is_grad = jnp.where(row >= CAP, 1, 0)
    slot = (row - CAP * is_grad).astype(F32)
    kind = 2 * in_half + is_grad
    first = jnp.where(lax.broadcasted_iota(jnp.int32, shape, 2) == 0, 1.0, 0.0)

    def packed(t):
        return pltpu.make_async_copy(
            pack_s.at[t % 2], send.at[t // 8, at((t % 8) * block, block)], pack_sem.at[t % 2]
        )

    def go(t):
        packed(t).wait()
        w, low = t // 8, (t % 8) * block

        @pl.loop(low, jnp.minimum(low + block, devices - 1))
        def _(n):
            pltpu.make_async_remote_copy(
                send.at[w, at(n)],
                came.at[w, at(n)],
                f_send.at[w],
                f_recv.at[w * 4 + n // group],
                device_id=device_at(n, 1),
                device_id_type=MESH,
            ).start()

        @pl.when(t % 8 == 7)
        def _():
            last = at(devices - 1)
            pltpu.make_async_copy(send.at[w, last], came.at[w, last], f_recv.at[w * 4 + 3]).start()

    @pl.loop(0, 16)
    def _(t):
        w = t // 8
        these = pl.ds(pl.multiple_of((t % 8) * block, block), block)
        table = jnp.broadcast_to(tab_s[w, these, :][:, None, :], shape)
        weight = jnp.broadcast_to(wt_s[w, these, :][:, None, :], shape)
        pick = jnp.where(table == slot, 1.0, 0.0)
        scale = jnp.sum(jnp.where(is_grad == 1, pick * weight, first), axis=2, keepdims=True).reshape(block * 24, 1)
        pieces = [jnp.where(kind == m, pick, 0.0).reshape(block * 24, tokens).astype(BF) for m in range(4)]
        pack_s[t % 2] = (dot(jnp.concatenate(pieces, axis=1), src_s[...]) * scale).astype(BF)
        packed(t).start()

        @pl.when(t > 0)
        def _():
            go(t - 1)

    go(15)

    for c in loads:
        c.wait()
    pltpu.make_async_copy(gain_s, gain_s, gain_recv).wait()
    gain_ref[...] = jnp.concatenate([gain_s[i] for i in range(16)], axis=1)
    gsum_s[...] = jnp.zeros_like(gsum_s)

    @pl.loop(0, 8)
    def _(step):
        w, g = step // 4, step % 4
        slab = at(g * group, group)
        pltpu.make_async_copy(came.at[w, slab], came.at[w, slab], f_recv.at[step]).wait()
        load = pltpu.make_async_copy(came.at[w, slab], rows_s, load_sem)
        load.start()
        load.wait()
        mine = pl.ds(pl.multiple_of(g * rows, rows), rows)
        for b in range(4):
            moved = dot(into_ref[...], rows_s[b * 192 : (b + 1) * 192, :])
            there = pl.ds(pl.multiple_of(g * rows + b * 48, 16), 48)
            for h in range(2):
                raw_s[b * 48 : (b + 1) * 48, h * half : (h + 1) * half] = moved[h * 48 : (h + 1) * 48, :]
                grad_s[w, there, h * half : (h + 1) * half] = moved[96 + h * 48 : 96 + (h + 1) * 48, :].astype(BF)
        raw = raw_s[...]
        root = lax.rsqrt(jnp.mean(raw * raw, axis=1, keepdims=True) + EPSILON)
        normed = (raw * root * gain_ref[...]).astype(BF)
        norm_s[w, mine, :] = normed
        pre_gate = dot(normed, g_gate[w])
        pre_up = dot(normed, g_up[w])
        sig = jax.nn.sigmoid(pre_gate)
        silu = pre_gate * sig
        act_s[w, mine, :] = (silu * pre_up).astype(BF)
        grad_act = dot(grad_s[w, mine, :], g_down[w], 1, 1)
        gate_back = (grad_act * pre_up * sig * (1.0 + pre_gate * (1.0 - sig))).astype(BF)
        up_back = (grad_act * silu).astype(BF)
        gb_s[w, mine, :] = gate_back
        ub_s[w, mine, :] = up_back
        returned = (dot(gate_back, g_gate[w], 1, 1) + dot(up_back, g_up[w], 1, 1)).astype(BF)
        gsum_s[...] += jnp.sum(returned.astype(F32) * (raw_s[...] * root), axis=0, keepdims=True)
        for b in range(4):
            part = returned[b * 48 : (b + 1) * 48, :]
            stacked = jnp.concatenate([part[:, q * quarter : (q + 1) * quarter] for q in range(4)], axis=0)
            ret_s[b * 192 : (b + 1) * 192, :] = dot(out_of_ref[...], stacked).astype(BF)
        store = pltpu.make_async_copy(ret_s, ret.at[w, slab], store_sem)
        store.start()
        store.wait()

        @pl.loop(g * group, jnp.minimum(g * group + group, devices - 1))
        def _(n):
            pltpu.make_async_remote_copy(
                ret.at[w, at(n)],
                back.at[w, at(n)],
                r_send,
                r_recv.at[step],
                device_id=device_at(n, -1),
                device_id_type=MESH,
            ).start()

    for w in range(2):
        last = at(devices - 1)
        pltpu.make_async_copy(ret.at[w, last], back.at[w, last], r_recv.at[w * 4 + 3]).start()

    for p in range(16):
        piece_s[p] = gsum_s[:, p * 128 : (p + 1) * 128]

    def piece(i):
        return pltpu.make_async_remote_copy(
            piece_s.at[(dp + i) % 16], arrive_s.at[i], t_send.at[0], t_recv.at[0],
            device_id=((dp + i) % 16, seq), device_id_type=MESH,
        )

    @pl.loop(1, 16)
    def _(i):
        piece(i).start()

    wide = 256
    for w in range(2):
        if w == 1:
            for c in stores:
                c.wait()

        @pl.loop(0, width // wide)
        def _(j):
            lanes = pl.ds(pl.multiple_of(j * wide, wide), wide)
            left = norm_s[w, :, lanes]
            dw_s[0, lanes, :] = dot(left, gb_s[w], 0, 0).astype(BF)
            dw_s[1, lanes, :] = dot(left, ub_s[w], 0, 0).astype(BF)
            dd_s[:, lanes] = dot(act_s[w], grad_s[w, :, lanes], 0, 0).astype(BF)

        stores = [
            pltpu.make_async_copy(dw_s.at[0], d_gate.at[w], dw_sem.at[0]),
            pltpu.make_async_copy(dw_s.at[1], d_up.at[w], dw_sem.at[1]),
            pltpu.make_async_copy(dd_s, d_down.at[w], dw_sem.at[2]),
        ]
        for c in stores:
            c.start()

    fifteen = arrive_s.at[pl.ds(1, 15)]
    pltpu.make_async_copy(fifteen, fifteen, t_recv.at[0]).wait()
    share = piece_s[dp]
    for i in range(1, 16):
        share = share + arrive_s[i]
    share_s[...] = share

    def to_copy(i):
        return pltpu.make_async_remote_copy(
            share_s, share_in_s.at[i], t_send.at[1], t_recv.at[1], device_id=(dp, (seq + i) % 8), device_id_type=MESH
        )

    @pl.loop(1, 8)
    def _(i):
        to_copy(i).start()

    for c in stores:
        c.wait()

    sum_s[...] = jnp.zeros_like(sum_s)
    count = block * 24
    spread_at = lax.broadcasted_iota(jnp.int32, (block, count), 1) - 24 * lax.broadcasted_iota(
        jnp.int32, (block, count), 0
    )
    spread = jnp.where((spread_at >= 0) & (spread_at < 24), 1.0, 0.0).astype(BF)

    @pl.loop(0, 8)
    def _(step):
        w, g = step // 4, step % 4
        slab = at(g * group, group)
        pltpu.make_async_copy(back.at[w, slab], back.at[w, slab], r_recv.at[step]).wait()
        load = pltpu.make_async_copy(back.at[w, slab], back_s, load_sem)
        load.start()
        load.wait()
        for b in range(2):
            these = pl.ds(pl.multiple_of(g * group + b * block, block), block)
            table = dot(tab_s[w, these, :].astype(BF), spread, 0, 0)
            pick = jnp.where(table == slot_ref[...], 1.0, 0.0)
            left = jnp.concatenate(
                [jnp.where(part_ref[...] == float(q), pick, 0.0).astype(BF) for q in range(4)], axis=0
            )
            sum_s[...] += dot(left, back_s[b * count : (b + 1) * count, :])

    summed = jnp.concatenate([sum_s[q * tokens : (q + 1) * tokens, :] for q in range(4)], axis=1)
    raw = hid_ref[...].astype(F32)
    root = lax.rsqrt(jnp.mean(raw * raw, axis=1, keepdims=True) + EPSILON)
    scaled = raw * root
    gained = summed * gain_ref[...]
    centre = jnp.mean(gained * scaled, axis=1, keepdims=True)
    hidden_ref[...] = (cot_ref[...].astype(F32) + root * (gained - scaled * centre)).astype(BF)

    seven = share_in_s.at[pl.ds(1, 7)]
    pltpu.make_async_copy(seven, seven, t_recv.at[1]).wait()
    for i in range(1, 8):
        share = share + share_in_s[i]
    total_ref[...] = share

    most = at(0, devices - 1)
    for w in range(2):
        pltpu.make_async_copy(send.at[w, most], send.at[w, most], f_send.at[w]).wait()
        pltpu.make_async_copy(ret.at[w, most], ret.at[w, most], r_send).wait()
    pltpu.make_async_copy(fifteen, fifteen, t_send.at[0]).wait()
    pltpu.make_async_copy(seven, seven, t_send.at[1]).wait()
    pltpu.make_async_copy(gain_s.at[pl.ds(1, 15)], gain_s.at[pl.ds(1, 15)], gain_send).wait()


def core(ids_t, w_t, dest, hidden, cot, gain, gate, up, down):
    tokens, width = hidden.shape
    experts, _, deep = gate.shape
    devices = dest.shape[0]
    total = devices * 24
    slots, half = total // 4, width // 2
    hbm = pl.BlockSpec(memory_space=pl.ANY)
    vmem = pl.BlockSpec(memory_space=pltpu.VMEM)
    back = jax.ShapeDtypeStruct((2, total, width // 4), BF)
    rows = jax.ShapeDtypeStruct((2, total, half), BF)
    dma = pltpu.SemaphoreType.DMA
    place_in = np.arange(16 * 24) % 24
    slot = jnp.asarray((place_in % CAP)[None, :], F32)
    part = jnp.asarray((place_in // CAP)[None, :], F32)
    outs = pl.pallas_call(
        core_kernel,
        out_shape=[
            jax.ShapeDtypeStruct((tokens, width), BF),
            jax.ShapeDtypeStruct((1, 128), F32),
            back,
            back,
            rows,
            rows,
            jax.ShapeDtypeStruct(gate.shape, BF),
            jax.ShapeDtypeStruct(up.shape, BF),
            jax.ShapeDtypeStruct(down.shape, BF),
        ],
        in_specs=[vmem] * 5 + [hbm] * 4 + [vmem] * 4,
        out_specs=[vmem] * 2 + [hbm] * 7,
        scratch_shapes=[
            pltpu.VMEM((2, devices, tokens), F32),
            pltpu.VMEM((2, devices, tokens), F32),
            pltpu.VMEM((4 * tokens, half), BF),
            pltpu.VMEM((2, 16 * 24, half), BF),
            pltpu.VMEM((total // 4, width // 4), BF),
            pltpu.VMEM((4 * tokens, width // 4), F32),
            pltpu.VMEM((1, width), F32),
            pltpu.VMEM((16, 1, 128), F32),
            pltpu.VMEM(gate.shape, BF),
            pltpu.VMEM(up.shape, BF),
            pltpu.VMEM(down.shape, BF),
            pltpu.VMEM((slots // 4, width), F32),
            pltpu.VMEM((total // 4, half), BF),
            pltpu.VMEM((experts, slots, width), BF),
            pltpu.VMEM((experts, slots, width), BF),
            pltpu.VMEM((experts, slots, deep), BF),
            pltpu.VMEM((experts, slots, deep), BF),
            pltpu.VMEM((experts, slots, deep), BF),
            pltpu.VMEM((total // 4, width // 4), BF),
            pltpu.VMEM((2, width, deep), BF),
            pltpu.VMEM((deep, width), BF),
            pltpu.VMEM((1, width), F32),
            pltpu.VMEM((16, 1, 128), F32),
            pltpu.VMEM((16, 1, 128), F32),
            pltpu.VMEM((1, 128), F32),
            pltpu.VMEM((8, 1, 128), F32),
            dma((2,)), dma((3,)), dma, dma, dma((2,)), dma((8,)), dma, dma((8,)), dma, dma, dma((3,)), dma((2,)), dma((2,)),
        ],
        compiler_params=pltpu.CompilerParams(has_side_effects=True, vmem_limit_bytes=VMEM_LIMIT),
        cost_estimate=pl.CostEstimate(flops=60 * 10**9, bytes_accessed=80 * 10**6, transcendentals=10**6),
        name="core",
    )(
        ids_t, w_t, dest, hidden, cot, gain, gate, up, down,
        jnp.asarray(order_in(), BF), jnp.asarray(order_out(), BF), slot, part,
    )
    return outs[0], outs[1], outs[6], outs[7], outs[8]


def shards(
    hidden_in, cotangent, norm_gain, route_weights, expert_ids, expert_gate, expert_up, expert_down
):
    hidden, cot = hidden_in[0], cotangent[0]
    tokens, width = hidden.shape
    devices = lax.axis_size("dp") * lax.axis_size("seq")
    ids_t = expert_ids[0].T
    w_t = route_weights[0].T
    dp, seq = device_at(jnp.arange(devices, dtype=jnp.int32), 1)
    dest = (dp * 8 + seq).astype(jnp.int32).reshape(devices, 1)
    grad_hidden, grad_gain, grad_gate, grad_up, grad_down = core(
        ids_t, w_t, dest, hidden, cot, norm_gain.reshape(1, -1), expert_gate, expert_up, expert_down
    )
    return grad_hidden[None], grad_gain.reshape(-1), grad_gate, grad_up, grad_down


def solution(mesh):
    rows = P("dp", "seq", None)
    experts = P(("dp", "seq"), None, None)
    return jax.shard_map(
        shards,
        mesh=mesh,
        in_specs=(rows, rows, P("dp"), rows, rows, experts, experts, experts),
        out_specs=(rows, P("dp"), experts, experts, experts),
        check_vma=False,
    )
```

```python
import jax
import jax.numpy as jnp
import numpy as np
from jax import lax
from jax.experimental import pallas as pl
from jax.experimental.pallas import tpu as pltpu
from jax.sharding import PartitionSpec as P

TOP = 10
EPSILON = 1e-06
CAP = 6
BF = jnp.bfloat16
F32 = jnp.float32
VMEM_LIMIT = 63 * 2**20
MESH = pl.DeviceIdType.MESH
PART = ((0, 640), (640, 640), (1280, 768))
PLANE = ((1, 2), (0, 2), (0, 1))
LINE = 4 * CAP
ROWS = 16 * LINE
CHUNKS = 4


def dot(a, b, ca=1, cb=0):
    return lax.dot_general(a, b, (((ca,), (cb,)), ((), ())), preferred_element_type=F32)


def device_at(shift, core):
    dp, seq = lax.axis_index("dp"), lax.axis_index("seq")
    x, y, z = (dp + shift[0] + 4) % 4, (dp // 4 + shift[1] + 4) % 4, (seq // 2 + shift[2] + 4) % 4
    return y * 4 + x, z * 2 + (seq + core) % 2


def along(a, m):
    return tuple(m if i == a else 0 for i in range(3))


def across(a, p, sign):
    shift = [0, 0, 0]
    shift[PLANE[a][0]] = sign * (p // 4)
    shift[PLANE[a][1]] = sign * (p % 4)
    return tuple(shift)


def order(a):
    matrix = np.zeros((ROWS, ROWS), np.float32)
    for p in range(16):
        for m in range(4):
            at = [0, 0, 0]
            at[PLANE[a][0]], at[PLANE[a][1]], at[a] = p // 4, p % 4, m
            for j in range(CAP):
                matrix[(at[0] * 16 + at[1] * 4 + at[2]) * CAP + j, p * LINE + m * CAP + j] = 1
    return matrix


def core_kernel(
    meta_ref, dest_ref, hid_ref, cot_ref, gain_in, gate, up, down, order_ref, slot_ref, part_ref,
    hidden_ref, total_ref,
    send0, send1, send2, came0, came1, came2, ret0, ret1, ret2, back0, back1, back2, d_gate, d_up, d_down,
    meta_s, tab_s, wt_s, row0, row1, row2, cot0, cot1, cot2, pack0, pack1, pack2, in0, in1, in2, sum0, sum1, sum2,
    near0, near1, near2,
    gain_ref, gain_s, g_gate, g_up, g_down, raw_s, norm_s, grad_s, act_s, gb_s, ub_s,
    gsum_s, piece_s, arrive_s, share_s, share_in_s,
    ag_send, ag_recv, pack_sem, w_sem, gain_send, gain_recv, f_send, f_recv, r_send, r_recv, load_sem, dw_sem,
    t_send, t_recv, l_send, l_recv,
):
    dp, seq = lax.axis_index("dp"), lax.axis_index("seq")
    send, came, ret, back = (send0, send1, send2), (came0, came1, came2), (ret0, ret1, ret2), (back0, back1, back2)
    line_rows, line_cots, pack = (row0, row1, row2), (cot0, cot1, cot2), (pack0, pack1, pack2)
    into, sums, near = (in0, in1, in2), (sum0, sum1, sum2), (near0, near1, near2)
    tokens, width = hid_ref.shape

    for m in (2, 1, 3):
        for a in range(3):
            target = dict(device_id=device_at(along(a, m), 0), device_id_type=MESH)
            lanes = pl.ds(*PART[a])
            pltpu.make_async_remote_copy(meta_ref, meta_s.at[a, m], ag_send.at[3 * a + 0], ag_recv.at[3 * a + 0], **target).start()
            pltpu.make_async_remote_copy(hid_ref.at[:, lanes], line_rows[a].at[m], ag_send.at[3 * a + 1], ag_recv.at[3 * a + 1], **target).start()
            pltpu.make_async_remote_copy(cot_ref.at[:, lanes], line_cots[a].at[m], ag_send.at[3 * a + 2], ag_recv.at[3 * a + 2], **target).start()

    def gain_copy(i):
        return pltpu.make_async_remote_copy(
            gain_in, gain_s.at[dp], gain_send, gain_recv, device_id=((dp + i) % 16, seq), device_id_type=MESH
        )

    own_gain = pltpu.make_async_copy(gain_in, gain_s.at[dp], gain_recv)
    own_gain.start()

    @pl.loop(1, 16)
    def _(i):
        gain_copy(i).start()

    loads = [
        pltpu.make_async_copy(gate, g_gate, w_sem.at[0]),
        pltpu.make_async_copy(up, g_up, w_sem.at[1]),
        pltpu.make_async_copy(down, g_down, w_sem.at[2]),
    ]
    for c in loads:
        c.start()

    earlier = lax.broadcasted_iota(jnp.int32, (tokens, tokens), 0) < lax.broadcasted_iota(
        jnp.int32, (tokens, tokens), 1
    )
    before = jnp.where(earlier, 1.0, 0.0).astype(BF)
    for a in range(3):
        lanes = slice(PART[a][0], PART[a][0] + PART[a][1])
        meta_s[a, 0] = meta_ref[...]
        line_rows[a][0] = hid_ref[:, lanes]
        line_cots[a][0] = cot_ref[:, lanes]
    three = pl.ds(1, 3)
    for a in range(3):
        for n, ref in enumerate((meta_s.at[a, three], line_rows[a].at[three], line_cots[a].at[three])):
            pltpu.make_async_copy(ref, ref, ag_recv.at[3 * a + n]).wait()
        expert = jnp.broadcast_to(dest_ref[a], (CHUNKS * 16, tokens))
        for m in range(4):
            hit = jnp.zeros((CHUNKS * 16, tokens), F32)
            weight = jnp.zeros((CHUNKS * 16, tokens), F32)
            for k in range(TOP):
                same = meta_s[a, m, k : k + 1, :] == expert
                hit = hit + jnp.where(same, 1.0, 0.0)
                weight = weight + jnp.where(same, meta_s[a, m, 12 + k : 13 + k, :], 0.0)
            tab_s[a, m] = jnp.where(hit > 0.0, dot(hit.astype(BF), before), -1.0)
            wt_s[a, m] = weight

    def at(p, size=1):
        return pl.ds(pl.multiple_of(p * LINE, 8), size * LINE)

    shape = (16, LINE, tokens)
    row = lax.broadcasted_iota(jnp.int32, shape, 1)
    member = sum(jnp.where(row >= m * CAP, 1, 0) for m in range(1, 4))
    slot = (row - CAP * member).astype(F32)

    def forth(a, c, p):
        return pltpu.make_async_remote_copy(
            send[a].at[c, :, at(p)], came[a].at[c, :, at(p)], f_send.at[c * 3 + a], f_recv.at[c * 3 + a],
            device_id=device_at(across(a, p, 1), c % 2), device_id_type=MESH,
        )

    def forth_again(a, c, p):
        return pltpu.make_async_remote_copy(
            ret[a].at[c, at(p)], back[a].at[c, at(p)], r_send.at[c * 3 + a], r_recv.at[c * 3 + a],
            device_id=device_at(across(a, p, -1), c % 2), device_id_type=MESH,
        )

    def scattered(i):
        return ((i + 1) * 5) % 16

    @pl.loop(0, CHUNKS)
    def _(c):
        these = pl.ds(pl.multiple_of(c * 16, 16), 16)
        for a in range(3):
            pieces, scale = [], jnp.zeros((16, LINE, 1), F32)
            for m in range(4):
                table = jnp.broadcast_to(tab_s[a, m, these, :][:, None, :], shape)
                weight = jnp.broadcast_to(wt_s[a, m, these, :][:, None, :], shape)
                pick = jnp.where((member == m) & (table == slot), 1.0, 0.0)
                scale = scale + jnp.sum(pick * weight, axis=2, keepdims=True)
                pieces.append(pick.reshape(ROWS, tokens).astype(BF))
            left = jnp.concatenate(pieces, axis=1)
            size = PART[a][1]
            pack[a][0] = dot(left, line_rows[a][...].reshape(4 * tokens, size)).astype(BF)
            pack[a][1] = (dot(left, line_cots[a][...].reshape(4 * tokens, size)) * scale.reshape(ROWS, 1)).astype(BF)
            pltpu.make_async_copy(pack[a], send[a].at[c], pack_sem.at[a]).start()
        for a in range(3):
            pltpu.make_async_copy(pack[a], send[a].at[c], pack_sem.at[a]).wait()

        @pl.loop(0, 15)
        def _(i):
            for a in range(3):
                forth(a, c, scattered(i)).start()

        @pl.when(c % 2 == 1)
        def _():
            for a in range(3):
                forth(a, c, 0).start()

        @pl.when(c % 2 == 0)
        def _():
            for a in range(3):
                pltpu.make_async_copy(send[a].at[c, :, at(0)], came[a].at[c, :, at(0)], f_recv.at[c * 3 + a]).start()

    for c in loads:
        c.wait()
    pltpu.make_async_copy(gain_s, gain_s, gain_recv).wait()
    gain_ref[...] = jnp.concatenate([gain_s[i] for i in range(16)], axis=1)
    gsum_s[...] = jnp.zeros_like(gsum_s)
    wide = 256

    @pl.loop(0, CHUNKS)
    def _(c):
        w = c // 2
        for a in range(3):
            pltpu.make_async_copy(came[a].at[c], came[a].at[c], f_recv.at[c * 3 + a]).wait()
        for a in range(3):
            pltpu.make_async_copy(came[a].at[c], into[a], load_sem.at[a]).start()
        mine = pl.ds(pl.multiple_of((c % 2) * ROWS, ROWS), ROWS)
        for a in range(3):
            pltpu.make_async_copy(came[a].at[c], into[a], load_sem.at[a]).wait()
            lanes = slice(PART[a][0], PART[a][0] + PART[a][1])
            raw_s[:, lanes] = dot(order_ref[a], into[a][0])
            grad_s[w, mine, lanes] = dot(order_ref[a], into[a][1]).astype(BF)
        root = lax.rsqrt(jnp.mean(raw_s[...] * raw_s[...], axis=1, keepdims=True) + EPSILON)
        norm_s[w, mine, :] = (raw_s[...] * root * gain_ref[...]).astype(BF)
        pre_gate = dot(norm_s[w, mine, :], g_gate[w])
        pre_up = dot(norm_s[w, mine, :], g_up[w])
        sig = jax.nn.sigmoid(pre_gate)
        silu = pre_gate * sig
        act_s[w, mine, :] = (silu * pre_up).astype(BF)
        grad_act = dot(grad_s[w, mine, :], g_down[w], 1, 1)
        gb_s[w, mine, :] = (grad_act * pre_up * sig * (1.0 + pre_gate * (1.0 - sig))).astype(BF)
        ub_s[w, mine, :] = (grad_act * silu).astype(BF)
        for a in range(3):
            lanes = slice(PART[a][0], PART[a][0] + PART[a][1])
            returned = (
                dot(gb_s[w, mine, :], g_gate[w, lanes, :], 1, 1) + dot(ub_s[w, mine, :], g_up[w, lanes, :], 1, 1)
            ).astype(BF)
            gsum_s[:, lanes] += jnp.sum(returned.astype(F32) * (raw_s[:, lanes] * root), axis=0, keepdims=True)
            pack[a][0] = dot(order_ref[a], returned, 0, 0).astype(BF)
            pltpu.make_async_copy(pack[a].at[0], ret[a].at[c], pack_sem.at[a]).start()
        for a in range(3):
            pltpu.make_async_copy(pack[a].at[0], ret[a].at[c], pack_sem.at[a]).wait()

        @pl.loop(0, 15)
        def _(i):
            for a in range(3):
                forth_again(a, c, scattered(i)).start()

        @pl.when(c % 2 == 1)
        def _():
            for a in range(3):
                forth_again(a, c, 0).start()

            @pl.loop(0, width // wide)
            def _(j):
                lanes = pl.ds(pl.multiple_of(j * wide, wide), wide)
                left = norm_s[w, :, lanes]
                g_gate[w, lanes, :] = dot(left, gb_s[w], 0, 0).astype(BF)
                g_up[w, lanes, :] = dot(left, ub_s[w], 0, 0).astype(BF)
                g_down[w, :, lanes] = dot(act_s[w], grad_s[w, :, lanes], 0, 0).astype(BF)

            for n, (here, there) in enumerate(((g_gate, d_gate), (g_up, d_up), (g_down, d_down))):
                pltpu.make_async_copy(here.at[w], there.at[w], dw_sem.at[w * 3 + n]).start()

        @pl.when(c % 2 == 0)
        def _():
            for a in range(3):
                pltpu.make_async_copy(ret[a].at[c, at(0)], back[a].at[c, at(0)], r_recv.at[c * 3 + a]).start()

    for p in range(16):
        piece_s[p] = gsum_s[:, p * 128 : (p + 1) * 128]

    def piece(i):
        return pltpu.make_async_remote_copy(
            piece_s.at[(dp + i) % 16], arrive_s.at[i], t_send.at[0], t_recv.at[0],
            device_id=((dp + i) % 16, seq), device_id_type=MESH,
        )

    @pl.loop(1, 16)
    def _(i):
        piece(i).start()

    for a in range(3):
        sums[a][...] = jnp.zeros_like(sums[a])
    spread_at = lax.broadcasted_iota(jnp.int32, (16, ROWS), 1) - LINE * lax.broadcasted_iota(jnp.int32, (16, ROWS), 0)
    spread = jnp.where((spread_at >= 0) & (spread_at < LINE), 1.0, 0.0).astype(BF)

    @pl.loop(0, CHUNKS)
    def _(c):
        these = pl.ds(pl.multiple_of(c * 16, 16), 16)
        for a in range(3):
            pltpu.make_async_copy(back[a].at[c], back[a].at[c], r_recv.at[c * 3 + a]).wait()
        for a in range(3):
            pltpu.make_async_copy(back[a].at[c], into[a].at[0], load_sem.at[a]).start()
        for a in range(3):
            pieces = []
            for m in range(4):
                table = dot(tab_s[a, m, these, :].astype(BF), spread, 0, 0)
                pieces.append(
                    jnp.where((part_ref[...] == float(m)) & (table == slot_ref[...]), 1.0, 0.0).astype(BF)
                )
            left = jnp.concatenate(pieces, axis=0)
            pltpu.make_async_copy(back[a].at[c], into[a].at[0], load_sem.at[a]).wait()
            sums[a][...] += dot(left, into[a][0])

    for a in range(3):
        line_rows[a][...] = sums[a][...].reshape(4, tokens, PART[a][1]).astype(BF)
    for m in (2, 1, 3):
        for a in range(3):
            pltpu.make_async_remote_copy(
                line_rows[a].at[m], near[a].at[m], l_send.at[a], l_recv.at[a],
                device_id=device_at(along(a, -m), 0), device_id_type=MESH,
            ).start()

    fifteen = arrive_s.at[pl.ds(1, 15)]
    pltpu.make_async_copy(fifteen, fifteen, t_recv.at[0]).wait()
    share = piece_s[dp]
    for i in range(1, 16):
        share = share + arrive_s[i]
    share_s[...] = share

    def to_copy(i):
        return pltpu.make_async_remote_copy(
            share_s, share_in_s.at[i], t_send.at[1], t_recv.at[1], device_id=(dp, (seq + i) % 8), device_id_type=MESH
        )

    @pl.loop(1, 8)
    def _(i):
        to_copy(i).start()

    for a in range(3):
        pltpu.make_async_copy(near[a].at[three], near[a].at[three], l_recv.at[a]).wait()
    summed = jnp.concatenate(
        [
            sums[a][0:tokens, :] + near[a][1].astype(F32) + near[a][2].astype(F32) + near[a][3].astype(F32)
            for a in range(3)
        ],
        axis=1,
    )
    raw = hid_ref[...].astype(F32)
    root = lax.rsqrt(jnp.mean(raw * raw, axis=1, keepdims=True) + EPSILON)
    scaled = raw * root
    gained = summed * gain_ref[...]
    centre = jnp.mean(gained * scaled, axis=1, keepdims=True)
    hidden_ref[...] = (cot_ref[...].astype(F32) + root * (gained - scaled * centre)).astype(BF)

    seven = share_in_s.at[pl.ds(1, 7)]
    pltpu.make_async_copy(seven, seven, t_recv.at[1]).wait()
    for i in range(1, 8):
        share = share + share_in_s[i]
    total_ref[...] = share

    for w in range(2):
        for n, (here, there) in enumerate(((g_gate, d_gate), (g_up, d_up), (g_down, d_down))):
            pltpu.make_async_copy(here.at[w], there.at[w], dw_sem.at[w * 3 + n]).wait()
    for a in range(3):
        for n, ref in enumerate((meta_s.at[a, three], line_rows[a].at[three], line_cots[a].at[three])):
            pltpu.make_async_copy(ref, ref, ag_send.at[3 * a + n]).wait()
        pltpu.make_async_copy(near[a].at[three], near[a].at[three], l_send.at[a]).wait()
        for c in range(CHUNKS):
            sent = at(0, 16) if c % 2 == 1 else at(1, 15)
            pltpu.make_async_copy(send[a].at[c, :, sent], send[a].at[c, :, sent], f_send.at[c * 3 + a]).wait()
            pltpu.make_async_copy(ret[a].at[c, sent], ret[a].at[c, sent], r_send.at[c * 3 + a]).wait()
    pltpu.make_async_copy(fifteen, fifteen, t_send.at[0]).wait()
    pltpu.make_async_copy(seven, seven, t_send.at[1]).wait()
    pltpu.make_async_copy(gain_s.at[pl.ds(1, 15)], gain_s.at[pl.ds(1, 15)], gain_send).wait()


def core(meta, dest, hidden, cot, gain, gate, up, down):
    tokens, width = hidden.shape
    experts, _, deep = gate.shape
    slots = 2 * ROWS
    hbm = pl.BlockSpec(memory_space=pl.ANY)
    vmem = pl.BlockSpec(memory_space=pltpu.VMEM)
    dma = pltpu.SemaphoreType.DMA
    sizes = [size for _, size in PART]
    shape = jax.ShapeDtypeStruct
    pairs = [shape((CHUNKS, 2, ROWS, size), BF) for size in sizes]
    singles = [shape((CHUNKS, ROWS, size), BF) for size in sizes]
    place = np.arange(ROWS) % LINE
    slot = jnp.asarray((place % CAP)[None, :], F32)
    part = jnp.asarray((place // CAP)[None, :], F32)
    line = [pltpu.VMEM((4, tokens, size), BF) for size in sizes]
    both = [pltpu.VMEM((2, ROWS, size), BF) for size in sizes]
    outs = pl.pallas_call(
        core_kernel,
        out_shape=[shape((tokens, width), BF), shape((1, 128), F32)]
        + pairs * 2
        + singles * 2
        + [shape(gate.shape, BF), shape(up.shape, BF), shape(down.shape, BF)],
        in_specs=[vmem] * 4 + [hbm] * 4 + [vmem] * 3,
        out_specs=[vmem] * 2 + [hbm] * 15,
        scratch_shapes=[
            pltpu.VMEM((3, 4, 24, tokens), F32),
            pltpu.VMEM((3, 4, CHUNKS * 16, tokens), F32),
            pltpu.VMEM((3, 4, CHUNKS * 16, tokens), F32),
        ]
        + line * 2
        + both * 2
        + [pltpu.VMEM((4 * tokens, size), F32) for size in sizes]
        + line
        + [
            pltpu.VMEM((1, width), F32),
            pltpu.VMEM((16, 1, 128), F32),
            pltpu.VMEM(gate.shape, BF),
            pltpu.VMEM(up.shape, BF),
            pltpu.VMEM(down.shape, BF),
            pltpu.VMEM((ROWS, width), F32),
            pltpu.VMEM((experts, slots, width), BF),
            pltpu.VMEM((experts, slots, width), BF),
            pltpu.VMEM((experts, slots, deep), BF),
            pltpu.VMEM((experts, slots, deep), BF),
            pltpu.VMEM((experts, slots, deep), BF),
            pltpu.VMEM((1, width), F32),
            pltpu.VMEM((16, 1, 128), F32),
            pltpu.VMEM((16, 1, 128), F32),
            pltpu.VMEM((1, 128), F32),
            pltpu.VMEM((8, 1, 128), F32),
            dma((9,)), dma((9,)), dma((3,)), dma((3,)), dma, dma, dma((12,)), dma((12,)), dma((12,)), dma((12,)),
            dma((3,)), dma((6,)), dma((2,)), dma((2,)), dma((3,)), dma((3,)),
        ],
        compiler_params=pltpu.CompilerParams(has_side_effects=True, vmem_limit_bytes=VMEM_LIMIT),
        cost_estimate=pl.CostEstimate(flops=60 * 10**9, bytes_accessed=80 * 10**6, transcendentals=10**6),
        name="core",
    )(
        meta, dest, hidden, cot, gain, gate, up, down,
        jnp.asarray(np.stack([order(a) for a in range(3)]), BF), slot, part,
    )
    return outs[0], outs[1], outs[-3], outs[-2], outs[-1]


def shards(
    hidden_in, cotangent, norm_gain, route_weights, expert_ids, expert_gate, expert_up, expert_down
):
    zeros = jnp.zeros((2, hidden_in.shape[1]), F32)
    meta = jnp.concatenate([expert_ids[0].T.astype(F32), zeros, route_weights[0].T, zeros], axis=0)
    n = jnp.arange(CHUNKS * 16, dtype=jnp.int32)
    dest = []
    for a in range(3):
        dp, seq = device_at(across(a, n % 16, 1), (n // 16) % 2)
        dest.append(2 * (dp * 8 + seq) + n // 32)
    dest = jnp.stack(dest).astype(F32)[:, :, None]
    grad_hidden, grad_gain, grad_gate, grad_up, grad_down = core(
        meta, dest, hidden_in[0], cotangent[0], norm_gain.reshape(1, -1), expert_gate, expert_up, expert_down
    )
    return grad_hidden[None], grad_gain.reshape(-1), grad_gate, grad_up, grad_down


def solution(mesh):
    rows = P("dp", "seq", None)
    experts = P(("dp", "seq"), None, None)
    return jax.shard_map(
        shards,
        mesh=mesh,
        in_specs=(rows, rows, P("dp"), rows, rows, experts, experts, experts),
        out_specs=(rows, P("dp"), experts, experts, experts),
        check_vma=False,
    )
```

```python
import jax
import jax.numpy as jnp
import numpy as np
from jax import lax
from jax.experimental import pallas as pl
from jax.experimental.pallas import tpu as pltpu
from jax.sharding import PartitionSpec as P

TOP = 10
EPSILON = 1e-06
CAP = 6
BF = jnp.bfloat16
F32 = jnp.float32
VMEM_LIMIT = 63 * 2**20
MESH = pl.DeviceIdType.MESH
PART = ((0, 640), (640, 640), (1280, 768))
PLANE = ((1, 2), (0, 2), (0, 1))
LINE = 4 * CAP
BOTH = pl.ds(0, 2)
ROWS = 16 * LINE
CHUNKS = 4


def dot(a, b, ca=1, cb=0):
    return lax.dot_general(a, b, (((ca,), (cb,)), ((), ())), preferred_element_type=F32)


def device_at(shift, core):
    dp, seq = lax.axis_index("dp"), lax.axis_index("seq")
    x, y, z = (dp + shift[0] + 4) % 4, (dp // 4 + shift[1] + 4) % 4, (seq // 2 + shift[2] + 4) % 4
    return y * 4 + x, z * 2 + (seq + core) % 2


def along(a, m):
    return tuple(m if i == a else 0 for i in range(3))


def across(a, p, sign):
    shift = [0, 0, 0]
    shift[PLANE[a][0]] = sign * (p // 4)
    shift[PLANE[a][1]] = sign * (p % 4)
    return tuple(shift)


def order(a):
    matrix = np.zeros((ROWS, ROWS), np.float32)
    for p in range(16):
        for m in range(4):
            at = [0, 0, 0]
            at[PLANE[a][0]], at[PLANE[a][1]], at[a] = p // 4, p % 4, m
            for j in range(CAP):
                matrix[(at[0] * 16 + at[1] * 4 + at[2]) * CAP + j, p * LINE + m * CAP + j] = 1
    return matrix


def core_kernel(
    meta_ref, dest_ref, hid_ref, cot_ref, gain_in, gate, up, down, order_ref, slot_ref, part_ref,
    summed_ref, gain_ref, total_ref,
    send0, send1, send2, came0, came1, came2, ret0, ret1, ret2, back0, back1, back2, d_gate, d_up, d_down,
    meta_s, tab_s, wt_s, row0, row1, row2, cot0, cot1, cot2, pack0, pack1, pack2, in0, in1, in2, sum0, sum1, sum2,
    near0, near1, near2,
    gain_s, g_gate, g_up, g_down, raw_s, norm_s, grad_s, act_s, gb_s, ub_s,
    gsum_s, piece_s, arrive_s, share_s, share_in_s,
    ag_send, ag_recv, pack_sem, w_sem, gain_send, gain_recv, f_send, f_recv, r_send, r_recv, load_sem, dw_sem,
    t_send, t_recv, l_send, l_recv,
):
    dp, seq = lax.axis_index("dp"), lax.axis_index("seq")
    send, came, ret, back = (send0, send1, send2), (came0, came1, came2), (ret0, ret1, ret2), (back0, back1, back2)
    line_rows, line_cots, pack = (row0, row1, row2), (cot0, cot1, cot2), (pack0, pack1, pack2)
    into, sums, near = (in0, in1, in2), (sum0, sum1, sum2), (near0, near1, near2)
    tokens, width = hid_ref.shape

    for m in (2, 1, 3):
        for a in range(3):
            target = dict(device_id=device_at(along(a, m), 0), device_id_type=MESH)
            pltpu.make_async_remote_copy(meta_ref, meta_s.at[a, m], ag_send.at[3 * a + 0], ag_recv.at[3 * a + 0], **target).start()
    for n, (source, lines) in enumerate(((hid_ref, line_rows), (cot_ref, line_cots))):
        for m in (2, 1, 3):
            for a in range(3):
                pltpu.make_async_remote_copy(
                    source.at[:, pl.ds(*PART[a])], lines[a].at[m], ag_send.at[3 * a + 1 + n], ag_recv.at[3 * a + 1 + n],
                    device_id=device_at(along(a, m), 0), device_id_type=MESH,
                ).start()

    def gain_copy(i):
        return pltpu.make_async_remote_copy(
            gain_in, gain_s.at[dp], gain_send, gain_recv, device_id=((dp + i) % 16, seq), device_id_type=MESH
        )

    own_gain = pltpu.make_async_copy(gain_in, gain_s.at[dp], gain_recv)
    own_gain.start()

    @pl.loop(1, 16)
    def _(i):
        gain_copy(i).start()

    loads = [
        pltpu.make_async_copy(gate, g_gate, w_sem.at[0]),
        pltpu.make_async_copy(up, g_up, w_sem.at[1]),
        pltpu.make_async_copy(down, g_down, w_sem.at[2]),
    ]
    for c in loads:
        c.start()

    earlier = lax.broadcasted_iota(jnp.int32, (tokens, tokens), 0) < lax.broadcasted_iota(
        jnp.int32, (tokens, tokens), 1
    )
    before = jnp.where(earlier, 1.0, 0.0).astype(BF)
    for a in range(3):
        lanes = slice(PART[a][0], PART[a][0] + PART[a][1])
        meta_s[a, 0] = meta_ref[...]
        line_rows[a][0] = hid_ref[:, lanes]
        line_cots[a][0] = cot_ref[:, lanes]
    three = pl.ds(1, 3)

    def landed(a, n, ref):
        pltpu.make_async_copy(ref, ref, ag_recv.at[3 * a + n]).wait()

    for a in range(3):
        landed(a, 0, meta_s.at[a, three])
        expert = jnp.broadcast_to(dest_ref[a], (CHUNKS * 16, tokens))
        for m in range(4):
            hit = jnp.zeros((CHUNKS * 16, tokens), F32)
            weight = jnp.zeros((CHUNKS * 16, tokens), F32)
            for k in range(TOP):
                same = meta_s[a, m, k : k + 1, :] == expert
                hit = hit + jnp.where(same, 1.0, 0.0)
                weight = weight + jnp.where(same, meta_s[a, m, 12 + k : 13 + k, :], 0.0)
            tab_s[a, m] = jnp.where(hit > 0.0, dot(hit.astype(BF), before), -1.0)
            wt_s[a, m] = weight
    def at(p, size=1):
        return pl.ds(pl.multiple_of(p * LINE, 8), size * LINE)

    shape = (16, LINE, tokens)
    row = lax.broadcasted_iota(jnp.int32, shape, 1)
    member = sum(jnp.where(row >= m * CAP, 1, 0) for m in range(1, 4))
    slot = (row - CAP * member).astype(F32)

    def forth(a, c, p, kinds):
        return pltpu.make_async_remote_copy(
            send[a].at[c, kinds, at(p)], came[a].at[c, kinds, at(p)], f_send.at[c * 3 + a], f_recv.at[c * 3 + a],
            device_id=device_at(across(a, p, 1), c % 2), device_id_type=MESH,
        )

    def forth_again(a, c, p):
        return pltpu.make_async_remote_copy(
            ret[a].at[c, at(p)], back[a].at[c, at(p)], r_send.at[c * 3 + a], r_recv.at[c * 3 + a],
            device_id=device_at(across(a, p, -1), c % 2), device_id_type=MESH,
        )

    def scattered(i):
        return ((i + 1) * 7) % 16

    def picked(a, c):
        these = pl.ds(pl.multiple_of(c * 16, 16), 16)
        pieces, scale = [], jnp.zeros((16, LINE, 1), F32)
        for m in range(4):
            table = jnp.broadcast_to(tab_s[a, m, these, :][:, None, :], shape)
            weight = jnp.broadcast_to(wt_s[a, m, these, :][:, None, :], shape)
            pick = jnp.where((member == m) & (table == slot), 1.0, 0.0)
            scale = scale + jnp.sum(pick * weight, axis=2, keepdims=True)
            pieces.append(pick.reshape(ROWS, tokens).astype(BF))
        return jnp.concatenate(pieces, axis=1), scale.reshape(ROWS, 1)

    def packed(a, c, kind):
        return pltpu.make_async_copy(pack[a].at[kind], send[a].at[c, kind], pack_sem.at[2 * a + kind])

    def packing(c, kinds):
        for a in range(3):
            left, scale = picked(a, c)
            for kind in kinds:
                rows = dot(left, (line_rows, line_cots)[kind][a][...].reshape(4 * tokens, PART[a][1]))
                pack[a][kind] = (rows if kind == 0 else rows * scale).astype(BF)
                packed(a, c, kind).start()
        for a in range(3):
            for kind in kinds:
                packed(a, c, kind).wait()

    def issue(c):
        @pl.loop(0, 15)
        def _(i):
            for a in range(3):
                forth(a, c, scattered(i), BOTH).start()

        @pl.when(c % 2 == 1)
        def _():
            for a in range(3):
                forth(a, c, 0, BOTH).start()

        @pl.when(c % 2 == 0)
        def _():
            for a in range(3):
                pltpu.make_async_copy(send[a].at[c, :, at(0)], came[a].at[c, :, at(0)], f_recv.at[c * 3 + a]).start()

    for kind in range(2):
        for a in range(3):
            landed(a, 1 + kind, (line_rows, line_cots)[kind][a].at[three])
        packing(0, (kind,))

        @pl.loop(0, 15)
        def _(i):
            for a in range(3):
                forth(a, 0, scattered(i), pl.ds(kind, 1)).start()

        for a in range(3):
            own = (0, kind, at(0))
            pltpu.make_async_copy(send[a].at[own], came[a].at[own], f_recv.at[a]).start()

    @pl.loop(1, CHUNKS)
    def _(c):
        packing(c, (0, 1))
        issue(c)

    for c in loads:
        c.wait()
    pltpu.make_async_copy(gain_s, gain_s, gain_recv).wait()
    gain_ref[...] = jnp.concatenate([gain_s[i] for i in range(16)], axis=1)
    gsum_s[...] = jnp.zeros_like(gsum_s)
    wide = 256

    @pl.loop(0, CHUNKS)
    def _(c):
        w = c // 2
        for a in range(3):
            pltpu.make_async_copy(came[a].at[c], came[a].at[c], f_recv.at[c * 3 + a]).wait()
        for a in range(3):
            pltpu.make_async_copy(came[a].at[c], into[a], load_sem.at[a]).start()
        mine = pl.ds(pl.multiple_of((c % 2) * ROWS, ROWS), ROWS)
        for a in range(3):
            pltpu.make_async_copy(came[a].at[c], into[a], load_sem.at[a]).wait()
            lanes = slice(PART[a][0], PART[a][0] + PART[a][1])
            raw_s[:, lanes] = dot(order_ref[a], into[a][0])
            grad_s[w, mine, lanes] = dot(order_ref[a], into[a][1]).astype(BF)
        root = lax.rsqrt(jnp.mean(raw_s[...] * raw_s[...], axis=1, keepdims=True) + EPSILON)
        norm_s[w, mine, :] = (raw_s[...] * root * gain_ref[...]).astype(BF)
        pre_gate = dot(norm_s[w, mine, :], g_gate[w])
        pre_up = dot(norm_s[w, mine, :], g_up[w])
        sig = jax.nn.sigmoid(pre_gate)
        silu = pre_gate * sig
        act_s[w, mine, :] = (silu * pre_up).astype(BF)
        grad_act = dot(grad_s[w, mine, :], g_down[w], 1, 1)
        gb_s[w, mine, :] = (grad_act * pre_up * sig * (1.0 + pre_gate * (1.0 - sig))).astype(BF)
        ub_s[w, mine, :] = (grad_act * silu).astype(BF)
        for a in range(3):
            lanes = slice(PART[a][0], PART[a][0] + PART[a][1])
            returned = (
                dot(gb_s[w, mine, :], g_gate[w, lanes, :], 1, 1) + dot(ub_s[w, mine, :], g_up[w, lanes, :], 1, 1)
            ).astype(BF)
            gsum_s[:, lanes] += jnp.sum(returned.astype(F32) * (raw_s[:, lanes] * root), axis=0, keepdims=True)
            pack[a][0] = dot(order_ref[a], returned, 0, 0).astype(BF)
            pltpu.make_async_copy(pack[a].at[0], ret[a].at[c], pack_sem.at[a]).start()
        for a in range(3):
            pltpu.make_async_copy(pack[a].at[0], ret[a].at[c], pack_sem.at[a]).wait()

        @pl.loop(0, 15)
        def _(i):
            for a in range(3):
                forth_again(a, c, scattered(i)).start()

        @pl.when(c % 2 == 1)
        def _():
            for a in range(3):
                forth_again(a, c, 0).start()

            @pl.loop(0, width // wide)
            def _(j):
                lanes = pl.ds(pl.multiple_of(j * wide, wide), wide)
                left = norm_s[w, :, lanes]
                g_gate[w, lanes, :] = dot(left, gb_s[w], 0, 0).astype(BF)
                g_up[w, lanes, :] = dot(left, ub_s[w], 0, 0).astype(BF)
                g_down[w, :, lanes] = dot(act_s[w], grad_s[w, :, lanes], 0, 0).astype(BF)

            for n, (here, there) in enumerate(((g_gate, d_gate), (g_up, d_up), (g_down, d_down))):
                pltpu.make_async_copy(here.at[w], there.at[w], dw_sem.at[w * 3 + n]).start()

        @pl.when(c % 2 == 0)
        def _():
            for a in range(3):
                pltpu.make_async_copy(ret[a].at[c, at(0)], back[a].at[c, at(0)], r_recv.at[c * 3 + a]).start()

    for p in range(16):
        piece_s[p] = gsum_s[:, p * 128 : (p + 1) * 128]

    def piece(i):
        return pltpu.make_async_remote_copy(
            piece_s.at[(dp + i) % 16], arrive_s.at[i], t_send.at[0], t_recv.at[0],
            device_id=((dp + i) % 16, seq), device_id_type=MESH,
        )

    @pl.loop(1, 16)
    def _(i):
        piece(i).start()

    for a in range(3):
        sums[a][...] = jnp.zeros_like(sums[a])
    spread_at = lax.broadcasted_iota(jnp.int32, (16, ROWS), 1) - LINE * lax.broadcasted_iota(jnp.int32, (16, ROWS), 0)
    spread = jnp.where((spread_at >= 0) & (spread_at < LINE), 1.0, 0.0).astype(BF)

    def gathered(c, a):
        pltpu.make_async_copy(back[a].at[c], back[a].at[c], r_recv.at[c * 3 + a]).wait()
        load = pltpu.make_async_copy(back[a].at[c], into[a].at[0], load_sem.at[a])
        load.start()
        pieces = []
        for m in range(4):
            table = dot(tab_s[a, m, pl.ds(pl.multiple_of(c * 16, 16), 16), :].astype(BF), spread, 0, 0)
            pieces.append(jnp.where((part_ref[...] == float(m)) & (table == slot_ref[...]), 1.0, 0.0).astype(BF))
        left = jnp.concatenate(pieces, axis=0)
        load.wait()
        sums[a][...] += dot(left, into[a][0])

    @pl.loop(0, CHUNKS - 1)
    def _(c):
        for a in range(3):
            gathered(c, a)

    for a in range(3):
        gathered(CHUNKS - 1, a)
        line_rows[a][...] = sums[a][...].reshape(4, tokens, PART[a][1]).astype(BF)
        for m in (2, 1, 3):
            pltpu.make_async_remote_copy(
                line_rows[a].at[m], near[a].at[m], l_send.at[a], l_recv.at[a],
                device_id=device_at(along(a, -m), 0), device_id_type=MESH,
            ).start()

    fifteen = arrive_s.at[pl.ds(1, 15)]
    pltpu.make_async_copy(fifteen, fifteen, t_recv.at[0]).wait()
    share = piece_s[dp]
    for i in range(1, 16):
        share = share + arrive_s[i]
    share_s[...] = share

    def to_copy(i):
        return pltpu.make_async_remote_copy(
            share_s, share_in_s.at[i], t_send.at[1], t_recv.at[1], device_id=(dp, (seq + i) % 8), device_id_type=MESH
        )

    @pl.loop(1, 8)
    def _(i):
        to_copy(i).start()

    for a in range(3):
        pltpu.make_async_copy(near[a].at[three], near[a].at[three], l_recv.at[a]).wait()
    for a in range(3):
        lanes = slice(PART[a][0], PART[a][0] + PART[a][1])
        summed_ref[:, lanes] = (
            sums[a][0:tokens, :] + near[a][1].astype(F32) + near[a][2].astype(F32) + near[a][3].astype(F32)
        )

    seven = share_in_s.at[pl.ds(1, 7)]
    pltpu.make_async_copy(seven, seven, t_recv.at[1]).wait()
    for i in range(1, 8):
        share = share + share_in_s[i]
    total_ref[...] = share

    for w in range(2):
        for n, (here, there) in enumerate(((g_gate, d_gate), (g_up, d_up), (g_down, d_down))):
            pltpu.make_async_copy(here.at[w], there.at[w], dw_sem.at[w * 3 + n]).wait()
    for a in range(3):
        for n, ref in enumerate((meta_s.at[a, three], line_rows[a].at[three], line_cots[a].at[three])):
            pltpu.make_async_copy(ref, ref, ag_send.at[3 * a + n]).wait()
        pltpu.make_async_copy(near[a].at[three], near[a].at[three], l_send.at[a]).wait()
        for c in range(CHUNKS):
            sent = at(0, 16) if c % 2 == 1 else at(1, 15)
            pltpu.make_async_copy(send[a].at[c, :, sent], send[a].at[c, :, sent], f_send.at[c * 3 + a]).wait()
            pltpu.make_async_copy(ret[a].at[c, sent], ret[a].at[c, sent], r_send.at[c * 3 + a]).wait()
    pltpu.make_async_copy(fifteen, fifteen, t_send.at[0]).wait()
    pltpu.make_async_copy(seven, seven, t_send.at[1]).wait()
    pltpu.make_async_copy(gain_s.at[pl.ds(1, 15)], gain_s.at[pl.ds(1, 15)], gain_send).wait()


def core(meta, dest, hidden, cot, gain, gate, up, down):
    tokens, width = hidden.shape
    experts, _, deep = gate.shape
    slots = 2 * ROWS
    hbm = pl.BlockSpec(memory_space=pl.ANY)
    vmem = pl.BlockSpec(memory_space=pltpu.VMEM)
    dma = pltpu.SemaphoreType.DMA
    sizes = [size for _, size in PART]
    shape = jax.ShapeDtypeStruct
    pairs = [shape((CHUNKS, 2, ROWS, size), BF) for size in sizes]
    singles = [shape((CHUNKS, ROWS, size), BF) for size in sizes]
    place = np.arange(ROWS) % LINE
    slot = jnp.asarray((place % CAP)[None, :], F32)
    part = jnp.asarray((place // CAP)[None, :], F32)
    line = [pltpu.VMEM((4, tokens, size), BF) for size in sizes]
    both = [pltpu.VMEM((2, ROWS, size), BF) for size in sizes]
    outs = pl.pallas_call(
        core_kernel,
        out_shape=[shape((tokens, width), F32), shape((1, width), F32), shape((1, 128), F32)]
        + pairs * 2
        + singles * 2
        + [shape(gate.shape, BF), shape(up.shape, BF), shape(down.shape, BF)],
        in_specs=[vmem] * 4 + [hbm] * 4 + [vmem] * 3,
        out_specs=[vmem] * 3 + [hbm] * 15,
        scratch_shapes=[
            pltpu.VMEM((3, 4, 24, tokens), F32),
            pltpu.VMEM((3, 4, CHUNKS * 16, tokens), F32),
            pltpu.VMEM((3, 4, CHUNKS * 16, tokens), F32),
        ]
        + line * 2
        + both * 2
        + [pltpu.VMEM((4 * tokens, size), F32) for size in sizes]
        + line
        + [
            pltpu.VMEM((16, 1, 128), F32),
            pltpu.VMEM(gate.shape, BF),
            pltpu.VMEM(up.shape, BF),
            pltpu.VMEM(down.shape, BF),
            pltpu.VMEM((ROWS, width), F32),
            pltpu.VMEM((experts, slots, width), BF),
            pltpu.VMEM((experts, slots, width), BF),
            pltpu.VMEM((experts, slots, deep), BF),
            pltpu.VMEM((experts, slots, deep), BF),
            pltpu.VMEM((experts, slots, deep), BF),
            pltpu.VMEM((1, width), F32),
            pltpu.VMEM((16, 1, 128), F32),
            pltpu.VMEM((16, 1, 128), F32),
            pltpu.VMEM((1, 128), F32),
            pltpu.VMEM((8, 1, 128), F32),
            dma((9,)), dma((9,)), dma((6,)), dma((3,)), dma, dma, dma((12,)), dma((12,)), dma((12,)), dma((12,)),
            dma((3,)), dma((6,)), dma((2,)), dma((2,)), dma((3,)), dma((3,)),
        ],
        compiler_params=pltpu.CompilerParams(has_side_effects=True, vmem_limit_bytes=VMEM_LIMIT),
        cost_estimate=pl.CostEstimate(flops=60 * 10**9, bytes_accessed=80 * 10**6, transcendentals=10**6),
        name="core",
    )(
        meta, dest, hidden, cot, gain, gate, up, down,
        jnp.asarray(np.stack([order(a) for a in range(3)]), BF), slot, part,
    )
    return outs[:3], outs[-3:]


def finish_kernel(
    summed_ref, gain_ref, total_ref, hid_ref, cot_ref, gate, up, down,
    hidden_ref, share_ref, d_gate, d_up, d_down, gate_s, up_s, down_s, in_sem, out_sem,
):
    moves = [(gate, gate_s, d_gate), (up, up_s, d_up), (down, down_s, d_down)]
    pieces = [
        (
            pltpu.make_async_copy(src.at[w], mid.at[w], in_sem.at[w, n]),
            pltpu.make_async_copy(mid.at[w], out.at[w], out_sem.at[w, n]),
        )
        for w in range(2)
        for n, (src, mid, out) in enumerate(moves)
    ]
    for into, _ in pieces:
        into.start()
    raw = hid_ref[...].astype(F32)
    root = lax.rsqrt(jnp.mean(raw * raw, axis=1, keepdims=True) + EPSILON)
    scaled = raw * root
    gained = summed_ref[...] * gain_ref[...]
    centre = jnp.mean(gained * scaled, axis=1, keepdims=True)
    for into, out in pieces:
        into.wait()
        out.start()
    hidden_ref[...] = (cot_ref[...].astype(F32) + root * (gained - scaled * centre)).astype(BF)
    share_ref[...] = total_ref[...]
    for _, out in pieces:
        out.wait()


def finish(sums, hidden, cot, grads):
    hbm = pl.BlockSpec(memory_space=pl.ANY)
    vmem = pl.BlockSpec(memory_space=pltpu.VMEM)
    shape = lambda x: jax.ShapeDtypeStruct(x.shape, x.dtype)
    return pl.pallas_call(
        finish_kernel,
        out_shape=[shape(hidden), shape(sums[2])] + [shape(g) for g in grads],
        in_specs=[vmem] * 5 + [hbm] * 3,
        out_specs=[vmem] * 2 + [hbm] * 3,
        scratch_shapes=[pltpu.VMEM(g.shape, BF) for g in grads]
        + [pltpu.SemaphoreType.DMA((2, 3)), pltpu.SemaphoreType.DMA((2, 3))],
        compiler_params=pltpu.CompilerParams(vmem_limit_bytes=VMEM_LIMIT),
        cost_estimate=pl.CostEstimate(flops=10**7, bytes_accessed=27 * 10**6, transcendentals=0),
        name="finish",
    )(*sums, hidden, cot, *grads)


def shards(
    hidden_in, cotangent, norm_gain, route_weights, expert_ids, expert_gate, expert_up, expert_down
):
    zeros = jnp.zeros((2, hidden_in.shape[1]), F32)
    meta = jnp.concatenate([expert_ids[0].T.astype(F32), zeros, route_weights[0].T, zeros], axis=0)
    n = jnp.arange(CHUNKS * 16, dtype=jnp.int32)
    dest = []
    for a in range(3):
        dp, seq = device_at(across(a, n % 16, 1), (n // 16) % 2)
        dest.append(2 * (dp * 8 + seq) + n // 32)
    dest = jnp.stack(dest).astype(F32)[:, :, None]
    hidden, cot = hidden_in[0], cotangent[0]
    sums, grads = core(meta, dest, hidden, cot, norm_gain.reshape(1, -1), expert_gate, expert_up, expert_down)
    grad_hidden, grad_gain, grad_gate, grad_up, grad_down = finish(sums, hidden, cot, grads)
    return grad_hidden[None], grad_gain.reshape(-1), grad_gate, grad_up, grad_down


def solution(mesh):
    rows = P("dp", "seq", None)
    experts = P(("dp", "seq"), None, None)
    return jax.shard_map(
        shards,
        mesh=mesh,
        in_specs=(rows, rows, P("dp"), rows, rows, experts, experts, experts),
        out_specs=(rows, P("dp"), experts, experts, experts),
        check_vma=False,
    )
```
